128 devices in a mesh: dp: 4 (over x), expert: 32 (over z, y, core).
Axes of the slice: x: 4, y: 4, z: 4, core: 2. Of those that a mesh axis runs over, the one named last changes fastest.
Arguments:
- tokens: bfloat16 [32, 512, 4096], P('expert', 'dp'), may hold values from -6 to 6
- w_gate: bfloat16 [32, 4096, 896], P('expert'), may hold values from -0.09375 to 0.09375
- w_up: bfloat16 [32, 4096, 896], P('expert'), may hold values from -0.09375 to 0.09375
- w_down: bfloat16 [32, 896, 4096], P('expert'), may hold values from -0.1875 to 0.1875
- expert_ids: int32 [32, 512, 4], P('expert'), may hold values from 0 to 31, all different within a row
- gate_index: int32 [32, 512, 4], P('expert'), may hold values from 0 to 255
- gate_table: float32 [256], replicated, may hold values from 0.05 to 1
- spill: int32 [32, 512], P('expert'), may hold values from 0 to 3, as said below
Outputs:
- mixed: bfloat16 [32, 512, 4096], P('expert', 'dp')
The draws below stay inside these ranges and needn't reach their ends.
Inputs may be any that keep to these rules, and one draw needn't show every extreme that they name: `spill`: A token is dispatched by a device of its own column. Of the 128 tokens of one device at most 32 are dispatched by any one other device, and in every draw some device hands exactly 32 to some peer.
All inputs are finite; a program needn't handle non-finite values.
Results may differ from the reference program's by a relative error of at most 0.0058.
Values may be sent and summed in bfloat16 or wider, within the bound.
No kernel may reach another device: no remote copies, remote signals or barrier semaphores. Data moves between devices by JAX's collectives and lax.ppermute only.
A program may use at most 128 MiB of HBM per device.

```python
import math
import jax
import jax.numpy as jnp
from jax import lax

D = 4096
FF = 896
TOP = 4
LEVELS = 256
TOK_DEV = 128
EXPERTS = 32
NCOL = 32
COL_TOK = 512
CAP = 24
SPILL = 32
N_DP = 4


def draw_spill(key, part):

    def column(column_key):
        count_key, perm_key, pick_key = jax.random.split(column_key, 3)
        counts = jax.random.randint(count_key, (N_DP, N_DP - 1), 0, SPILL + 1)
        full_home = jax.random.randint(pick_key, (), 0, N_DP)
        counts = counts.at[full_home, 0].set(SPILL)
        bounds = jnp.cumsum(counts, axis=1)
        positions = jax.vmap(lambda home_key: jax.random.permutation(home_key, TOK_DEV))(jax.random.split(perm_key, N_DP))
        passed = jnp.sum((positions[:, :, None] >= bounds[:, None, :]).astype(jnp.int32), axis=2)
        home_dev = jnp.arange(N_DP, dtype=jnp.int32)[:, None]
        senders = jnp.where(passed < N_DP - 1, (home_dev + 1 + passed) % N_DP, home_dev)
        return senders.reshape(-1).astype(jnp.int32)
    column_keys = jax.random.split(jax.random.fold_in(key, 17), NCOL)
    return jax.vmap(column)(column_keys)


def with_ends(result, stream_key, least, top_value):
    spot = [jax.random.randint(jax.random.fold_in(stream_key, axis), (), 0, length) for axis, length in enumerate(result.shape)]
    longest = result.shape.index(max(result.shape))
    next_to = spot[:longest] + [(spot[longest] + 1) % result.shape[longest]] + spot[longest + 1:]
    return result.at[tuple(spot)].set(least).at[tuple(next_to)].set(top_value)


def steps_of(stream_key, dims, pieces, low, largest):
    level = 1.0
    for position, parts in pieces:
        steps = jax.random.uniform(jax.random.fold_in(jax.random.fold_in(stream_key, 6), position), (parts,), jnp.float32, low / len(pieces), largest / len(pieces))
        level = level * jnp.repeat(jnp.exp(steps), dims[position] // parts).reshape((-1,) + (1,) * (len(dims) - 1 - position))
    return level


def different_ones(own_key, rows, number_of, top, lift):
    order = jax.random.permutation(jax.random.fold_in(own_key, 1), number_of)
    pull = order
    for power in range(3):
        pull = pull * pull // number_of
    pull = pull * lift // number_of
    chance = jax.random.randint(jax.random.fold_in(own_key, 2), (rows, number_of), 0, 4096) + pull
    fixed_rows = jax.random.permutation(jax.random.fold_in(own_key, 3), rows)[jnp.arange(number_of) % rows]
    chance = jnp.where(jnp.arange(rows)[:, None] == fixed_rows[None, :], 1 << 14, chance)
    priority = chance * number_of + jnp.arange(number_of)
    return lax.top_k(priority.astype(jnp.int32), top)[1].astype(jnp.int32)


def bell_draw(stream_key, shape, spread, bound, cuts=(), kind=jnp.bfloat16):
    values = jax.random.normal(stream_key, shape, jnp.float32) * spread
    if len(cuts) > 0:
        values = steps_of(stream_key, shape, cuts, -0.22, 0.18) * values
    return jnp.clip(values, min=-bound, max=bound).astype(kind)


def setup_inputs(seed: int = 0) -> dict:
    seeds = jax.random.split(jax.random.key(seed), 9)
    tokens = bell_draw(seeds[0], (NCOL, COL_TOK, D), 1.0, 6.0, ((0, 32), (1, 4)))
    w_gate = bell_draw(seeds[1], (EXPERTS, D, FF), D ** -0.5, 0.09375, ((0, 32),))
    w_up = bell_draw(seeds[2], (EXPERTS, D, FF), D ** -0.5, 0.09375, ((0, 32),))
    w_down = bell_draw(seeds[3], (EXPERTS, FF, D), FF ** -0.5, 0.1875, ((0, 32),))
    expert_ids = different_ones(seeds[4], NCOL * COL_TOK, EXPERTS, TOP, 2048).reshape((NCOL, COL_TOK, TOP))
    gate_index = with_ends(jax.random.randint(seeds[5], (NCOL, COL_TOK, TOP), 0, LEVELS), jax.random.fold_in(seeds[5], 1), 0, LEVELS - 1).astype(jnp.int32)
    gate_table = jnp.clip(jnp.exp(jax.random.uniform(seeds[6], (LEVELS,), jnp.float32, math.log(0.05), math.log(1.0))), 0.05, 1.0)
    spill = draw_spill(jax.random.fold_in(seeds[8], 71), 0)
    return dict(tokens=tokens, w_gate=w_gate, w_up=w_up, w_down=w_down, expert_ids=expert_ids, gate_index=gate_index, gate_table=gate_table, spill=spill)


def rank_within(route_row, key_count):
    onehot = (route_row[:, None] == jnp.arange(key_count, dtype=jnp.int32)[None, :]).astype(jnp.int32)
    return jnp.sum((jnp.cumsum(onehot, axis=0) - onehot) * onehot, axis=1).astype(jnp.int32)


def reference(tokens, w_gate, w_up, w_down, expert_ids, gate_index, gate_table, spill):
    ncol_count = tokens.shape[0]
    column_tokens = tokens.shape[1]
    model_width = tokens.shape[2]
    experts_all = w_gate.shape[0]
    top_count = expert_ids.shape[2]
    picked = gate_table[gate_index]
    weight = picked / jnp.sum(picked, axis=-1, keepdims=True)
    pair_sender = jnp.repeat(spill, top_count, axis=1).astype(jnp.int32)
    flat_ids = expert_ids.reshape(ncol_count, column_tokens * top_count).astype(jnp.int32)
    route_key = pair_sender * experts_all + flat_ids
    slot_rank = lax.map(lambda row: rank_within(row, N_DP * experts_all), route_key)
    is_kept = slot_rank < CAP
    per_expert = ncol_count * N_DP * CAP
    column_base = jnp.arange(ncol_count, dtype=jnp.int32)[:, None]
    slot_index = (column_base * N_DP + pair_sender) * CAP + slot_rank
    slot_index = jnp.where(is_kept, slot_index, per_expert).astype(jnp.int32)
    token_total = ncol_count * column_tokens
    pair_token = column_base * column_tokens + jnp.arange(column_tokens * top_count, dtype=jnp.int32)[None, :] // top_count
    row_source = jnp.full((experts_all, per_expert + 1), token_total, jnp.int32)
    row_source = row_source.at[flat_ids, slot_index].set(pair_token.astype(jnp.int32))[:, :per_expert]
    kept_weight = jnp.where(is_kept, weight.reshape(ncol_count, column_tokens * top_count), 0.0).astype(jnp.float32)
    row_scale = jnp.zeros((experts_all, per_expert + 1), jnp.float32)
    row_scale = row_scale.at[flat_ids, slot_index].set(kept_weight)[:, :per_expert]
    padded = jnp.concatenate([tokens.reshape(token_total, model_width), jnp.zeros((1, model_width), tokens.dtype)], axis=0)

    def expert_step(totals, inputs):
        gate_mat, up_mat, down_mat, sources, scales = inputs
        rows_in = padded[sources]
        gate_part = jnp.dot(rows_in, gate_mat, preferred_element_type=jnp.float32)
        up_part = jnp.dot(rows_in, up_mat, preferred_element_type=jnp.float32)
        hidden = (jax.nn.silu(gate_part) * up_part).astype(jnp.bfloat16)
        expert_out = jnp.dot(hidden, down_mat, preferred_element_type=jnp.float32).astype(jnp.bfloat16)
        totals = totals.at[sources].add(scales[:, None] * expert_out.astype(jnp.float32))
        return totals, None

    start = jnp.zeros((token_total + 1, model_width), jnp.float32)
    totals, unused = lax.scan(expert_step, start, (w_gate, w_up, w_down, row_source, row_scale))
    return totals[:token_total].astype(jnp.bfloat16).reshape(ncol_count, column_tokens, model_width)
```

```python
import functools
import jax
import jax.numpy as jnp
from jax import lax
from jax.experimental import pallas as pl
from jax.experimental.pallas import tpu as pltpu
from jax.sharding import PartitionSpec as P

F32 = jnp.float32
BF16 = jnp.bfloat16
I32 = jnp.int32


def onehot(mask):
    return jnp.where(mask, 1.0, 0.0).astype(BF16)


def strict_upper(n):
    return onehot(lax.broadcasted_iota(I32, (n, n), 0) < lax.broadcasted_iota(I32, (n, n), 1))


def dot(a, b):
    return jnp.dot(a, b, preferred_element_type=F32)


def dot_nt(a, b):
    return lax.dot_general(a, b, (((1,), (1,)), ((), ())), preferred_element_type=F32)


def dot_tn(a, b):
    return lax.dot_general(a, b, (((0,), (0,)), ((), ())), preferred_element_type=F32)


def spill_kernel(dp_count, room, me_ref, spill_ref, tok_ref, pick_ref, out_ref):
    own_rows = tok_ref.shape[0]
    slots = dp_count * room

    @pl.when(pl.program_id(0) == 0)
    def _():
        me = me_ref[0]
        senders = spill_ref[pl.ds(me, 1), :]
        peers = lax.broadcasted_iota(I32, (8, own_rows), 0)
        same = onehot(senders == peers)
        before = dot(same, strict_upper(own_rows))
        order = jnp.sum(before * same.astype(F32), axis=0, keepdims=True).astype(I32)
        target = jnp.where(senders == me, slots, senders * room + order)
        rows = lax.broadcasted_iota(I32, (slots, own_rows), 0)
        pick_ref[...] = onehot(rows == target)

    out_ref[...] = dot(pick_ref[...], tok_ref[...]).astype(BF16)


def slot_of(index, experts_all, first):
    rest = 8
    cut = experts_all * first
    in_first = index < cut
    expert = jnp.where(in_first, index // first, (index - cut) // rest)
    rank = jnp.where(in_first, index % first, first + (index - cut) % rest)
    return expert, rank + 1


def route_kernel(
    dp_count, room, experts_all, capacity, first, me_ref, spill_ref, ids_ref, weight_ref, pick_ref, high_ref, low_ref
):
    me = me_ref[0]
    own_rows = spill_ref.shape[1]
    top_count, column_tokens = ids_ref.shape
    source_rows = own_rows + dp_count * room
    slots = experts_all * capacity

    by_home = onehot(spill_ref[...] == me)
    order = dot(by_home, strict_upper(own_rows)).astype(I32)
    homes = lax.broadcasted_iota(I32, (dp_count, own_rows), 0)
    place = lax.broadcasted_iota(I32, (dp_count, own_rows), 1)
    row = jnp.where(homes == me, place, own_rows + homes * room + order)
    row = jnp.where(spill_ref[...] == me, row, source_rows)
    row = jnp.concatenate([row[h : h + 1] for h in range(dp_count)], axis=1)
    to_row = onehot(lax.broadcasted_iota(I32, (source_rows, column_tokens), 0) == row)

    experts = lax.broadcasted_iota(I32, (experts_all, column_tokens), 0)
    scale = jnp.zeros((experts_all, column_tokens), F32)
    chosen = jnp.zeros((experts_all, column_tokens), F32)
    mine = row < source_rows
    for k in range(top_count):
        hit = (ids_ref[k : k + 1, :] == experts) & mine
        scale = jnp.where(hit, weight_ref[k : k + 1, :], scale)
        chosen = jnp.where(hit, 1.0, chosen)
    rank = dot(chosen.astype(BF16), strict_upper(column_tokens))
    keep = (chosen > 0.0) & (rank < capacity)
    code = jnp.where(keep, rank + 1.0, 0.0).astype(BF16)
    scale = jnp.where(keep, scale, 0.0)
    high = scale.astype(BF16)
    low = (scale - high.astype(F32)).astype(BF16)

    slot_expert, slot_rank = slot_of(lax.broadcasted_iota(I32, (slots, experts_all), 0), experts_all, first)
    spread = onehot(slot_expert == lax.broadcasted_iota(I32, (slots, experts_all), 1))
    code_rows = dot_nt(code, to_row).astype(BF16)
    _, rank_col = slot_of(lax.broadcasted_iota(I32, (slots, source_rows), 0), experts_all, first)
    pick_ref[...] = onehot(dot(spread, code_rows).astype(I32) == rank_col)

    slot_expert, _ = slot_of(lax.broadcasted_iota(I32, (experts_all, slots), 1), experts_all, first)
    spread_t = onehot(slot_expert == lax.broadcasted_iota(I32, (experts_all, slots), 0))
    _, rank_row = slot_of(lax.broadcasted_iota(I32, (source_rows, slots), 1), experts_all, first)
    code_t = dot_nt(to_row, code).astype(BF16)
    filled = dot(code_t, spread_t).astype(I32) == rank_row
    high_t = dot(dot_nt(to_row, high).astype(BF16), spread_t)
    low_t = dot(dot_nt(to_row, low).astype(BF16), spread_t)
    high_ref[...] = jnp.where(filled, high_t, 0.0).astype(BF16)
    low_ref[...] = jnp.where(filled, low_t, 0.0).astype(BF16)


def build_kernel(pick_ref, tok_ref, arr_ref, out_ref):
    own_rows = tok_ref.shape[0]
    rows = dot(pick_ref[:, :own_rows], tok_ref[...]) + dot(pick_ref[:, own_rows:], arr_ref[...])
    out_ref[...] = rows.astype(BF16)


def combine_first_kernel(high_ref, low_ref, res_ref, out_ref):
    out_ref[...] = dot(high_ref[...], res_ref[...]) + dot(low_ref[...], res_ref[...])


def combine_rest_kernel(high_ref, low_ref, res_ref, part_ref, out_ref):
    total = part_ref[...] + dot(high_ref[...], res_ref[...]) + dot(low_ref[...], res_ref[...])
    out_ref[...] = total.astype(out_ref.dtype)


def finish_kernel(pick_ref, back_ref, own_ref, out_ref):
    out_ref[...] = (own_ref[...] + dot_tn(pick_ref[...], back_ref[...])).astype(BF16)


VM = pltpu.VMEM
LIMIT = 40 * 1024 * 1024


def whole(shape):
    return pl.BlockSpec(shape, lambda i: (0,) * len(shape))


def call(kernel, grid, in_specs, out_specs, out_shape, flops, size, name):
    return pl.pallas_call(
        kernel,
        grid=(grid,),
        in_specs=in_specs,
        out_specs=out_specs,
        out_shape=out_shape,
        name=name,
        compiler_params=pltpu.CompilerParams(dimension_semantics=("arbitrary",), vmem_limit_bytes=LIMIT),
        cost_estimate=pl.CostEstimate(flops=flops, bytes_accessed=size, transcendentals=0),
    )


def local(tokens, w_gate, w_up, w_down, expert_ids, gate_index, gate_table, spill):
    dp_count = lax.axis_size("dp")
    expert_count = lax.axis_size("expert")
    own_rows, width = tokens.shape[1:]
    column_tokens = spill.shape[1]
    top_count = expert_ids.shape[2]
    experts_all = w_gate.shape[0] * expert_count
    capacity = 3 * own_rows * top_count // (2 * experts_all)
    room = own_rows // 4
    moved = dp_count * room
    source_rows = own_rows + moved
    slots = experts_all * capacity
    first = capacity - 8
    cut = experts_all * first
    rest = slots - cut
    block = 1024
    grid = width // block
    me = lax.axis_index("dp").astype(I32).reshape(1)
    own = tokens[0]
    spill_rows = spill.reshape(dp_count, own_rows)
    smem = pl.BlockSpec(memory_space=pltpu.SMEM)
    sds = jax.ShapeDtypeStruct

    def cols(rows):
        return pl.BlockSpec((rows, block), lambda i: (0, i))

    give, outgoing = call(
        functools.partial(spill_kernel, dp_count, room),
        grid,
        [smem, whole((dp_count, own_rows)), cols(own_rows)],
        [whole((moved, own_rows)), cols(moved)],
        [sds((moved, own_rows), BF16), sds((moved, width), BF16)],
        2 * moved * own_rows * width,
        4 * own_rows * width,
        "spill_pick",
    )(me, spill_rows, own)
    arrived = lax.all_to_all(
        outgoing.reshape(dp_count, room, width), "dp", split_axis=0, concat_axis=0, tiled=True
    ).reshape(moved, width)

    level_count = gate_table.shape[0]
    index_t = gate_index[0].T
    ids_t = expert_ids[0].T
    matches = index_t[:, None, :] == jnp.arange(level_count, dtype=I32)[None, :, None]
    picked = jnp.sum(jnp.where(matches, gate_table[None, :, None], 0.0), axis=1)
    weight = picked / jnp.sum(picked, axis=0, keepdims=True)
    pick, high, low = call(
        functools.partial(route_kernel, dp_count, room, experts_all, capacity, first),
        1,
        [smem, whole((dp_count, own_rows)), whole((top_count, column_tokens)), whole((top_count, column_tokens))],
        [whole((slots, source_rows)), whole((source_rows, slots)), whole((source_rows, slots))],
        [sds((slots, source_rows), BF16), sds((source_rows, slots), BF16), sds((source_rows, slots), BF16)],
        2 * column_tokens * column_tokens * 600,
        3 * 2 * slots * source_rows,
        "route",
    )(me, spill_rows, ids_t, weight)

    def build(start, count, name):
        return call(
            build_kernel,
            grid,
            [pl.BlockSpec((count, source_rows), lambda i: (start // count, 0)), cols(own_rows), cols(moved)],
            cols(count),
            sds((count, width), BF16),
            2 * count * source_rows * width,
            2 * (count + source_rows) * width,
            name,
        )(pick, own, arrived)

    def exchange(rows):
        shaped = rows.reshape(expert_count, -1, width)
        return lax.all_to_all(shaped, "expert", split_axis=0, concat_axis=0, tiled=True).reshape(-1, width)

    def experts(rows):
        gate_part = dot(rows, w_gate[0])
        up_part = dot(rows, w_up[0])
        hidden = (jax.nn.silu(gate_part) * up_part).astype(BF16)
        return dot(hidden, w_down[0]).astype(BF16)

    block0 = exchange(build(0, cut, "build_first"))
    block1 = exchange(build(cut, rest, "build_rest"))
    back0 = exchange(experts(block0))
    back1 = exchange(experts(block1))

    part = call(
        combine_first_kernel,
        grid,
        [pl.BlockSpec((source_rows, cut), lambda i: (0, 0))] * 2 + [cols(cut)],
        cols(source_rows),
        sds((source_rows, width), F32),
        4 * source_rows * cut * width,
        2 * cut * width + 4 * source_rows * width,
        "combine_first",
    )(high, low, back0)

    def combine_rest(start, count, dtype, name):
        at = start // count
        weights = pl.BlockSpec((count, rest), lambda i: (at, cut // rest))
        return call(
            combine_rest_kernel,
            grid,
            [weights, weights, cols(rest), pl.BlockSpec((count, block), lambda i: (at, i))],
            cols(count),
            sds((count, width), dtype),
            4 * count * rest * width,
            2 * rest * width + 6 * count * width,
            name,
        )(high, low, back1, part)

    arrived_part = combine_rest(own_rows, moved, BF16, "combine_arrived")
    returned = lax.all_to_all(
        arrived_part.reshape(dp_count, room, width), "dp", split_axis=0, concat_axis=0, tiled=True
    ).reshape(moved, width)
    own_part = combine_rest(0, own_rows, F32, "combine_own")
    mixed = call(
        finish_kernel,
        grid,
        [whole((moved, own_rows)), cols(moved), cols(own_rows)],
        cols(own_rows),
        sds((own_rows, width), BF16),
        2 * moved * own_rows * width,
        8 * own_rows * width,
        "finish",
    )(give, returned, own_part)
    return mixed[None]


def solution(mesh):
    in_specs = (
        P("expert", "dp", None),
        P("expert", None, None),
        P("expert", None, None),
        P("expert", None, None),
        P("expert", None, None),
        P("expert", None, None),
        P(),
        P("expert", None),
    )
    out_specs = P("expert", "dp", None)
    return jax.shard_map(local, mesh=mesh, in_specs=in_specs, out_specs=out_specs, check_vma=False)
```

```python
import functools
import jax
import jax.numpy as jnp
from jax import lax
from jax.experimental import pallas as pl
from jax.experimental.pallas import tpu as pltpu
from jax.sharding import PartitionSpec as P

F32 = jnp.float32
BF16 = jnp.bfloat16
I32 = jnp.int32


def onehot(mask):
    return jnp.where(mask, 1.0, 0.0).astype(BF16)


def strict_upper(n):
    return onehot(lax.broadcasted_iota(I32, (n, n), 0) < lax.broadcasted_iota(I32, (n, n), 1))


def dot(a, b):
    return jnp.dot(a, b, preferred_element_type=F32)


def dot_nt(a, b):
    return lax.dot_general(a, b, (((1,), (1,)), ((), ())), preferred_element_type=F32)


def dot_tn(a, b):
    return lax.dot_general(a, b, (((0,), (0,)), ((), ())), preferred_element_type=F32)


def spill_kernel(dp_count, room, me_ref, spill_ref, tok_ref, pick_ref, *out_refs):
    own_rows = tok_ref.shape[0]
    slots = pick_ref.shape[0]

    @pl.when(pl.program_id(0) == 0)
    def _():
        me = me_ref[0]
        senders = spill_ref[pl.ds(me, 1), :]
        peers = lax.broadcasted_iota(I32, (8, own_rows), 0)
        same = onehot(senders == peers)
        before = dot(same, strict_upper(own_rows))
        order = jnp.sum(before * same.astype(F32), axis=0, keepdims=True).astype(I32)
        ahead = jnp.where(senders < me, senders - me + dp_count, senders - me)
        target = jnp.where(ahead == 0, slots, (ahead - 1) * room + order)
        rows = lax.broadcasted_iota(I32, (slots, own_rows), 0)
        pick_ref[...] = onehot(rows == target)

    picked = dot(pick_ref[...], tok_ref[...]).astype(BF16)
    for k, out_ref in enumerate(out_refs):
        out_ref[...] = picked[k * room : (k + 1) * room]


def slot_of(index, experts_all, first):
    rest = 8
    cut = experts_all * first
    in_first = index < cut
    expert = jnp.where(in_first, index // first, (index - cut) // rest)
    rank = jnp.where(in_first, index % first, first + (index - cut) % rest)
    return expert, rank + 1


def route_kernel(
    dp_count, room, experts_all, capacity, first, me_ref, spill_ref, ids_ref, weight_ref,
    pick_ref, high_own_ref, low_own_ref, high_arr_ref, low_arr_ref
):
    me = me_ref[0]
    own_rows = spill_ref.shape[1]
    top_count, column_tokens = ids_ref.shape
    source_rows = own_rows + (dp_count - 1) * room
    slots = experts_all * capacity

    by_home = onehot(spill_ref[...] == me)
    order = dot(by_home, strict_upper(own_rows)).astype(I32)
    homes = lax.broadcasted_iota(I32, (dp_count, own_rows), 0)
    place = lax.broadcasted_iota(I32, (dp_count, own_rows), 1)
    back = jnp.where(homes > me, me - homes + dp_count, me - homes)
    row = jnp.where(back == 0, place, own_rows + (back - 1) * room + order)
    row = jnp.where(spill_ref[...] == me, row, source_rows)
    row = jnp.concatenate([row[h : h + 1] for h in range(dp_count)], axis=1)
    to_row = onehot(lax.broadcasted_iota(I32, (source_rows, column_tokens), 0) == row)

    experts = lax.broadcasted_iota(I32, (experts_all, column_tokens), 0)
    scale = jnp.zeros((experts_all, column_tokens), F32)
    chosen = jnp.zeros((experts_all, column_tokens), F32)
    mine = row < source_rows
    for k in range(top_count):
        hit = (ids_ref[k : k + 1, :] == experts) & mine
        scale = jnp.where(hit, weight_ref[k : k + 1, :], scale)
        chosen = jnp.where(hit, 1.0, chosen)
    rank = dot(chosen.astype(BF16), strict_upper(column_tokens))
    keep = (chosen > 0.0) & (rank < capacity)
    code = jnp.where(keep, rank + 1.0, 0.0).astype(BF16)
    scale = jnp.where(keep, scale, 0.0)
    high = scale.astype(BF16)
    low = (scale - high.astype(F32)).astype(BF16)

    slot_expert, slot_rank = slot_of(lax.broadcasted_iota(I32, (slots, experts_all), 0), experts_all, first)
    spread = onehot(slot_expert == lax.broadcasted_iota(I32, (slots, experts_all), 1))
    code_rows = dot_nt(code, to_row).astype(BF16)
    _, rank_col = slot_of(lax.broadcasted_iota(I32, (slots, source_rows), 0), experts_all, first)
    pick_ref[...] = onehot(dot(spread, code_rows).astype(I32) == rank_col)

    slot_expert, _ = slot_of(lax.broadcasted_iota(I32, (experts_all, slots), 1), experts_all, first)
    spread_t = onehot(slot_expert == lax.broadcasted_iota(I32, (experts_all, slots), 0))
    _, rank_row = slot_of(lax.broadcasted_iota(I32, (source_rows, slots), 1), experts_all, first)
    code_t = dot_nt(to_row, code).astype(BF16)
    filled = dot(code_t, spread_t).astype(I32) == rank_row
    high_t = dot(dot_nt(to_row, high).astype(BF16), spread_t)
    low_t = dot(dot_nt(to_row, low).astype(BF16), spread_t)
    high_w = jnp.where(filled, high_t, 0.0).astype(BF16)
    low_w = jnp.where(filled, low_t, 0.0).astype(BF16)
    high_own_ref[...] = high_w[:own_rows]
    low_own_ref[...] = low_w[:own_rows]
    high_arr_ref[...] = high_w[own_rows:]
    low_arr_ref[...] = low_w[own_rows:]


def build_kernel(pick_ref, *refs):
    rows = jnp.concatenate([ref[...] for ref in refs[:-1]], axis=0)
    refs[-1][...] = dot(pick_ref[...], rows).astype(BF16)


def combine_first_kernel(high_own_ref, low_own_ref, high_arr_ref, low_arr_ref, res_ref, own_ref, arr_ref):
    own_ref[...] = dot(high_own_ref[...], res_ref[...]) + dot(low_own_ref[...], res_ref[...])
    arr_ref[...] = dot(high_arr_ref[...], res_ref[...]) + dot(low_arr_ref[...], res_ref[...])


def combine_own_kernel(high_ref, low_ref, res_ref, part_ref, out_ref):
    out_ref[...] = part_ref[...] + dot(high_ref[...], res_ref[...]) + dot(low_ref[...], res_ref[...])


def combine_arrived_kernel(room, high_ref, low_ref, res_ref, part_ref, *out_refs):
    total = part_ref[...] + dot(high_ref[...], res_ref[...]) + dot(low_ref[...], res_ref[...])
    for k, out_ref in enumerate(out_refs):
        out_ref[...] = total[k * room : (k + 1) * room].astype(BF16)


def finish_kernel(pick_ref, own_ref, *refs):
    back = jnp.concatenate([ref[...] for ref in refs[:-1]], axis=0)
    refs[-1][...] = (own_ref[...] + dot_tn(pick_ref[...], back)).astype(BF16)


GRANT = 32 * 1024 * 1024


def in_hbm(x):
    return pltpu.with_memory_space_constraint(x, pltpu.HBM)


def whole(shape):
    return pl.BlockSpec(shape, lambda i: (0,) * len(shape))


def call(kernel, grid, in_specs, out_specs, out_shape, flops, size, name):
    return pl.pallas_call(
        kernel,
        grid=(grid,),
        in_specs=in_specs,
        out_specs=out_specs,
        out_shape=out_shape,
        name=name,
        compiler_params=pltpu.CompilerParams(dimension_semantics=("arbitrary",), vmem_limit_bytes=GRANT),
        cost_estimate=pl.CostEstimate(flops=flops, bytes_accessed=size, transcendentals=0),
    )


def local(tokens, w_gate, w_up, w_down, expert_ids, gate_index, gate_table, spill):
    dp_count = lax.axis_size("dp")
    expert_count = lax.axis_size("expert")
    own_rows, width = tokens.shape[1:]
    column_tokens = spill.shape[1]
    top_count = expert_ids.shape[2]
    experts_all = w_gate.shape[0] * expert_count
    capacity = 3 * own_rows * top_count // (2 * experts_all)
    room = own_rows // 4
    moved = (dp_count - 1) * room
    source_rows = own_rows + moved
    slots = experts_all * capacity
    first = capacity - 8
    cut = experts_all * first
    rest = slots - cut
    block = 512
    grid = width // block
    me = lax.axis_index("dp").astype(I32).reshape(1)
    own = in_hbm(tokens[0])
    spill_rows = in_hbm(spill.reshape(dp_count, own_rows))
    smem = pl.BlockSpec(memory_space=pltpu.SMEM)
    sds = jax.ShapeDtypeStruct
    hbm = pltpu.HBM
    steps = range(1, dp_count)

    def cols(rows):
        return pl.BlockSpec((rows, block), lambda i: (0, i))

    def shift(blocks, sign):
        sent = {}
        for k in sorted(steps, key=lambda k: abs(dp_count - 2 * k)):
            pairs = [(i, (i + sign * k) % dp_count) for i in range(dp_count)]
            sent[k] = lax.ppermute(blocks[k - 1], "dp", pairs)
        return [sent[k] for k in steps]

    give, *outgoing = call(
        functools.partial(spill_kernel, dp_count, room),
        grid,
        [smem, whole((dp_count, own_rows)), cols(own_rows)],
        [whole((moved, own_rows))] + [cols(room)] * len(steps),
        [sds((moved, own_rows), BF16)] + [hbm((room, width), BF16)] * len(steps),
        2 * moved * own_rows * width,
        4 * own_rows * width,
        "spill_pick",
    )(me, spill_rows, own)
    arrived = shift(outgoing, 1)

    level_count = gate_table.shape[0]
    index_t = gate_index[0].T
    ids_t = in_hbm(expert_ids[0].T)
    matches = index_t[:, None, :] == jnp.arange(level_count, dtype=I32)[None, :, None]
    picked = jnp.sum(jnp.where(matches, gate_table[None, :, None], 0.0), axis=1)
    weight = picked / jnp.sum(picked, axis=0, keepdims=True)
    out_shapes = [(slots, source_rows)] + [(own_rows, slots)] * 2 + [(moved, slots)] * 2
    pick, high_own, low_own, high_arr, low_arr = call(
        functools.partial(route_kernel, dp_count, room, experts_all, capacity, first),
        1,
        [smem, whole((dp_count, own_rows)), whole((top_count, column_tokens)), whole((top_count, column_tokens))],
        [whole(shape) for shape in out_shapes],
        [sds(shape, BF16) for shape in out_shapes],
        2 * column_tokens * column_tokens * 600,
        3 * 2 * slots * source_rows,
        "route",
    )(me, spill_rows, ids_t, weight)

    def build(start, count, name):
        return call(
            build_kernel,
            grid,
            [pl.BlockSpec((count, source_rows), lambda i: (start // count, 0)), cols(own_rows)]
            + [cols(room)] * len(steps),
            cols(count),
            hbm((count, width), BF16),
            2 * count * source_rows * width,
            2 * (count + source_rows) * width,
            name,
        )(pick, own, *arrived)

    def exchange(rows):
        shaped = rows.reshape(expert_count, -1, width)
        return lax.all_to_all(shaped, "expert", split_axis=0, concat_axis=0, tiled=True).reshape(-1, width)

    def experts(rows):
        gate_part = dot(rows, w_gate[0])
        up_part = dot(rows, w_up[0])
        hidden = (jax.nn.silu(gate_part) * up_part).astype(BF16)
        return dot(hidden, w_down[0]).astype(BF16)

    block0 = exchange(build(0, cut, "build_first"))
    block1 = exchange(build(cut, rest, "build_rest"))
    back0 = exchange(experts(block0))
    back1 = exchange(experts(block1))

    def first_cols(rows):
        return pl.BlockSpec((rows, cut), lambda i: (0, 0))

    def rest_cols(rows):
        return pl.BlockSpec((rows, rest), lambda i: (0, cut // rest))

    part_own, part_arr = call(
        combine_first_kernel,
        grid,
        [first_cols(own_rows)] * 2 + [first_cols(moved)] * 2 + [cols(cut)],
        [cols(own_rows), cols(moved)],
        [hbm((own_rows, width), F32), hbm((moved, width), F32)],
        4 * source_rows * cut * width,
        2 * cut * width + 4 * source_rows * width,
        "combine_first",
    )(high_own, low_own, high_arr, low_arr, back0)
    arrived_parts = call(
        functools.partial(combine_arrived_kernel, room),
        grid,
        [rest_cols(moved)] * 2 + [cols(rest), cols(moved)],
        [cols(room)] * len(steps),
        [hbm((room, width), BF16)] * len(steps),
        4 * moved * rest * width,
        2 * rest * width + 6 * moved * width,
        "combine_arrived",
    )(high_arr, low_arr, back1, part_arr)
    returned = shift(arrived_parts, -1)
    own_part = call(
        combine_own_kernel,
        grid,
        [rest_cols(own_rows)] * 2 + [cols(rest), cols(own_rows)],
        cols(own_rows),
        sds((own_rows, width), F32),
        4 * own_rows * rest * width,
        2 * rest * width + 8 * own_rows * width,
        "combine_own",
    )(high_own, low_own, back1, part_own)
    mixed = call(
        finish_kernel,
        grid,
        [whole((moved, own_rows)), cols(own_rows)] + [cols(room)] * len(steps),
        cols(own_rows),
        sds((own_rows, width), BF16),
        2 * moved * own_rows * width,
        8 * own_rows * width,
        "finish",
    )(give, own_part, *returned)
    return mixed[None]


def solution(mesh):
    in_specs = (
        P("expert", "dp", None),
        P("expert", None, None),
        P("expert", None, None),
        P("expert", None, None),
        P("expert", None, None),
        P("expert", None, None),
        P(),
        P("expert", None),
    )
    out_specs = P("expert", "dp", None)
    return jax.shard_map(local, mesh=mesh, in_specs=in_specs, out_specs=out_specs, check_vma=False)
```

```python
import functools
import jax
import jax.numpy as jnp
from jax import lax
from jax.experimental import pallas as pl
from jax.experimental.pallas import tpu as pltpu
from jax.sharding import PartitionSpec as P

F32 = jnp.float32
BF16 = jnp.bfloat16
I32 = jnp.int32


def onehot(mask):
    return jnp.where(mask, 1.0, 0.0).astype(BF16)


def strict_upper(n):
    return onehot(lax.broadcasted_iota(I32, (n, n), 0) < lax.broadcasted_iota(I32, (n, n), 1))


def dot(a, b):
    return jnp.dot(a, b, preferred_element_type=F32)


def dot_nt(a, b):
    return lax.dot_general(a, b, (((1,), (1,)), ((), ())), preferred_element_type=F32)


def dot_tn(a, b):
    return lax.dot_general(a, b, (((0,), (0,)), ((), ())), preferred_element_type=F32)


def send(buf_ref, out_ref, sems, j):
    return pltpu.make_async_copy(buf_ref, out_ref, sems.at[j])


def parts(width, count):
    step = width // count
    return [pl.ds(j * step, step) for j in range(count)]


PIECES = 4


def spill_kernel(dp_count, room, me_ref, spill_ref, tok_ref, pick_ref, own_ref, *refs):
    out_refs, (spill_buf, buf, spill_sem, in_sems, out_sems) = refs[: dp_count - 1], refs[dp_count - 1 :]
    own_rows, width = tok_ref.shape
    slots = pick_ref.shape[0]
    load = pltpu.make_async_copy(spill_ref, spill_buf, spill_sem)
    load.start()
    cols = parts(width, PIECES)
    loads = [send(tok_ref.at[:, c], own_ref.at[:, c], in_sems, j) for j, c in enumerate(cols)]
    for copy in loads:
        copy.start()
    load.wait()
    me = me_ref[0]
    senders = spill_buf[pl.ds(me, 1), :]
    peers = lax.broadcasted_iota(I32, (8, own_rows), 0)
    same = onehot(senders == peers)
    before = dot(same, strict_upper(own_rows))
    order = jnp.sum(before * same.astype(F32), axis=0, keepdims=True).astype(I32)
    ahead = jnp.where(senders < me, senders - me + dp_count, senders - me)
    target = jnp.where(ahead == 0, slots, (ahead - 1) * room + order)
    rows = lax.broadcasted_iota(I32, (slots, own_rows), 0)
    pick = onehot(rows == target)
    pick_ref[...] = pick
    stores = []
    for j, c in enumerate(cols):
        loads[j].wait()
        buf[:, c] = dot(pick, own_ref[:, c]).astype(BF16)
        for k, out_ref in enumerate(out_refs):
            store = send(buf.at[pl.ds(k * room, room), c], out_ref.at[:, c], out_sems, j * len(out_refs) + k)
            store.start()
            stores.append(store)
    for store in stores:
        store.wait()


def slot_of(index, capacity):
    return index // capacity, index % capacity + 1


def route_kernel(
    dp_count, room, experts_all, capacity, me_ref, spill_ref, ids_ref, weight_ref,
    pick_ref, own_w_ref, arr_w_ref
):
    me = me_ref[0]
    own_rows = spill_ref.shape[1]
    top_count, column_tokens = ids_ref.shape
    source_rows = own_rows + (dp_count - 1) * room
    slots = experts_all * capacity

    by_home = onehot(spill_ref[...] == me)
    order = dot(by_home, strict_upper(own_rows)).astype(I32)
    homes = lax.broadcasted_iota(I32, (dp_count, own_rows), 0)
    place = lax.broadcasted_iota(I32, (dp_count, own_rows), 1)
    back = jnp.where(homes > me, me - homes + dp_count, me - homes)
    row = jnp.where(back == 0, place, own_rows + (back - 1) * room + order)
    row = jnp.where(spill_ref[...] == me, row, source_rows)
    row = jnp.concatenate([row[h : h + 1] for h in range(dp_count)], axis=1)
    to_row = onehot(lax.broadcasted_iota(I32, (source_rows, column_tokens), 0) == row)

    experts = lax.broadcasted_iota(I32, (experts_all, column_tokens), 0)
    scale = jnp.zeros((experts_all, column_tokens), F32)
    chosen = jnp.zeros((experts_all, column_tokens), F32)
    mine = row < source_rows
    for k in range(top_count):
        hit = (ids_ref[k : k + 1, :] == experts) & mine
        scale = jnp.where(hit, weight_ref[k : k + 1, :], scale)
        chosen = jnp.where(hit, 1.0, chosen)
    rank = dot(chosen.astype(BF16), strict_upper(column_tokens))
    keep = (chosen > 0.0) & (rank < capacity)
    code = jnp.where(keep, rank + 1.0, 0.0).astype(BF16)
    scale = jnp.where(keep, scale, 0.0)
    high = scale.astype(BF16)
    low = (scale - high.astype(F32)).astype(BF16)

    slot_expert, _ = slot_of(lax.broadcasted_iota(I32, (slots, experts_all), 0), capacity)
    spread = onehot(slot_expert == lax.broadcasted_iota(I32, (slots, experts_all), 1))
    code_rows = dot_nt(code, to_row).astype(BF16)
    _, rank_col = slot_of(lax.broadcasted_iota(I32, (slots, source_rows), 0), capacity)
    pick_ref[...] = onehot(dot(spread, code_rows).astype(I32) == rank_col)

    slot_expert, _ = slot_of(lax.broadcasted_iota(I32, (experts_all, slots), 1), capacity)
    spread_t = onehot(slot_expert == lax.broadcasted_iota(I32, (experts_all, slots), 0))
    _, rank_row = slot_of(lax.broadcasted_iota(I32, (source_rows, slots), 1), capacity)
    code_t = dot_nt(to_row, code).astype(BF16)
    filled = dot(code_t, spread_t).astype(I32) == rank_row
    high_t = dot(dot_nt(to_row, high).astype(BF16), spread_t)
    low_t = dot(dot_nt(to_row, low).astype(BF16), spread_t)
    high_w = jnp.where(filled, high_t, 0.0).astype(BF16)
    low_w = jnp.where(filled, low_t, 0.0).astype(BF16)
    own_w_ref[:own_rows] = high_w[:own_rows]
    own_w_ref[own_rows:] = low_w[:own_rows]
    arr_w_ref[: source_rows - own_rows] = high_w[own_rows:]
    arr_w_ref[source_rows - own_rows :] = low_w[own_rows:]


def build_kernel(pick_ref, *refs):
    *src_refs, out_ref, buf, sems = refs
    copies = []
    for j, c in enumerate(parts(out_ref.shape[1], PIECES)):
        rows = jnp.concatenate([ref[:, c] for ref in src_refs], axis=0)
        buf[:, c] = dot(pick_ref[...], rows).astype(BF16)
        copies.append(send(buf.at[:, c], out_ref.at[:, c], sems, j))
        copies[-1].start()
    for copy in copies:
        copy.wait()


GATE_COLS = 128
DOWN_COLS = 512


def ffn_kernel(x_in, gate_in, up_in, down_in, out_ref, x, both, down, acc, hidden, buf, x_sem, top_sem, both_sem, down_sem, out_sem):
    depth = x.shape[1] // PIECES
    tiles, downs = both.shape[0], down.shape[0]

    def lanes(n, size):
        return pl.ds(pl.multiple_of(n * size, size), size)

    def fetch(n):
        cols = lanes(n, GATE_COLS)
        return (
            pltpu.make_async_copy(gate_in.at[:, cols], both.at[n, :, pl.ds(0, GATE_COLS)], both_sem.at[n, 0]),
            pltpu.make_async_copy(up_in.at[:, cols], both.at[n, :, pl.ds(GATE_COLS, GATE_COLS)], both_sem.at[n, 1]),
        )

    def fetch_down(n):
        return pltpu.make_async_copy(down_in.at[:, lanes(n, DOWN_COLS)], down.at[n], down_sem.at[n])

    def store(n):
        return pltpu.make_async_copy(buf.at[n], out_ref.at[:, lanes(n, DOWN_COLS)], out_sem.at[n])

    def activate(n):
        gate_part, up_part = acc[:, :GATE_COLS], acc[:, GATE_COLS:]
        hidden[:, lanes(n, GATE_COLS)] = (jax.nn.silu(gate_part) * up_part).astype(BF16)

    top = []
    for k in range(PIECES):
        d = pl.ds(k * depth, depth)
        top.append((
            pltpu.make_async_copy(x_in.at[:, d], x.at[:, d], x_sem.at[k]),
            pltpu.make_async_copy(gate_in.at[d, pl.ds(0, GATE_COLS)], both.at[0, d, pl.ds(0, GATE_COLS)], top_sem.at[k, 0]),
            pltpu.make_async_copy(up_in.at[d, pl.ds(0, GATE_COLS)], both.at[0, d, pl.ds(GATE_COLS, GATE_COLS)], top_sem.at[k, 1]),
        ))
        for copy in top[-1]:
            copy.start()
    for n in (1, 2):
        for copy in fetch(n):
            copy.start()
    for k in range(PIECES):
        d = pl.ds(k * depth, depth)
        for copy in top[k]:
            copy.wait()
        part = dot(x[:, d], both[0, d, :])
        acc[...] = part if k == 0 else acc[...] + part
    activate(0)

    @pl.loop(1, tiles)
    def _(n):
        for copy in fetch(n):
            copy.wait()

        @pl.when(n + 2 < tiles)
        def _():
            for copy in fetch(n + 2):
                copy.start()

        @pl.when(n + 2 >= tiles)
        def _():
            half = (n + 2 - tiles) * (downs // 2)
            for j in range(downs // 2):
                fetch_down(half + j).start()

        acc[...] = dot(x[...], both[n])
        activate(n)

    @pl.loop(0, downs)
    def _(n):
        fetch_down(n).wait()
        buf[n] = dot(hidden[...], down[n]).astype(BF16)
        store(n).start()

    @pl.loop(0, downs)
    def _(n):
        store(n).wait()


def weighted(w_ref, res):
    both = dot(w_ref[...], res)
    half = both.shape[0] // 2
    return both[:half] + both[half:]


def each_piece(res_ref, res, sems):
    cols = parts(res.shape[1], PIECES)
    loads = [send(res_ref.at[:, c], res.at[:, c], sems, j) for j, c in enumerate(cols)]
    for load in loads:
        load.start()
    for j, c in enumerate(cols):
        loads[j].wait()
        yield j, c


def combine_own_kernel(w_ref, res_ref, out_ref, res, in_sems):
    for _, c in each_piece(res_ref, res, in_sems):
        out_ref[:, c] = weighted(w_ref, res[:, c])


def combine_arrived_kernel(room, w_ref, res_ref, *refs):
    *out_refs, res, buf, in_sems, sems = refs
    copies = []
    for j, c in each_piece(res_ref, res, in_sems):
        buf[:, c] = weighted(w_ref, res[:, c]).astype(BF16)
        for k, out_ref in enumerate(out_refs):
            copies.append(send(buf.at[pl.ds(k * room, room), c], out_ref.at[:, c], sems, j * len(out_refs) + k))
            copies[-1].start()
    for copy in copies:
        copy.wait()


def finish_kernel(pick_ref, own_ref, *refs):
    *back_refs, out_ref, buf, sems = refs
    copies = []
    for j, c in enumerate(parts(out_ref.shape[1], PIECES)):
        back = jnp.concatenate([ref[:, c] for ref in back_refs], axis=0)
        buf[:, c] = (own_ref[:, c] + dot_tn(pick_ref[...], back)).astype(BF16)
        copies.append(send(buf.at[:, c], out_ref.at[:, c], sems, j))
        copies[-1].start()
    for copy in copies:
        copy.wait()


GRANT = 24 * 1024 * 1024
FFN_GRANT = 56 * 1024 * 1024


def in_hbm(x):
    return pltpu.with_memory_space_constraint(x, pltpu.HBM)


VM = pl.BlockSpec(memory_space=pltpu.VMEM)
SM = pl.BlockSpec(memory_space=pltpu.SMEM)
HB = pl.BlockSpec(memory_space=pltpu.HBM)
DMA = pltpu.SemaphoreType.DMA


def call(kernel, in_specs, out_specs, out_shape, scratch, flops, size, name, grant=GRANT):
    return pl.pallas_call(
        kernel,
        in_specs=in_specs,
        out_specs=out_specs,
        out_shape=out_shape,
        scratch_shapes=scratch,
        name=name,
        compiler_params=pltpu.CompilerParams(vmem_limit_bytes=grant),
        cost_estimate=pl.CostEstimate(flops=flops, bytes_accessed=size, transcendentals=0),
    )


def local(tokens, w_gate, w_up, w_down, expert_ids, gate_index, gate_table, spill):
    dp_count = lax.axis_size("dp")
    expert_count = lax.axis_size("expert")
    own_rows, width = tokens.shape[1:]
    column_tokens = spill.shape[1]
    top_count = expert_ids.shape[2]
    experts_all = w_gate.shape[0] * expert_count
    capacity = 3 * own_rows * top_count // (2 * experts_all)
    room = own_rows // 4
    moved = (dp_count - 1) * room
    source_rows = own_rows + moved
    slots = experts_all * capacity
    ff = w_gate.shape[2]
    me = lax.axis_index("dp").astype(I32).reshape(1)
    own_in = in_hbm(tokens[0])
    spill_rows = spill.reshape(dp_count, own_rows)
    hbm, vmem = pltpu.HBM, pltpu.VMEM
    steps = range(1, dp_count)
    peers = len(steps)

    def shift(blocks, sign):
        sent = {}
        for k in sorted(steps, key=lambda k: abs(dp_count - 2 * k)):
            pairs = [(i, (i + sign * k) % dp_count) for i in range(dp_count)]
            sent[k] = lax.ppermute(blocks[k - 1], "dp", pairs)
        return [sent[k] for k in steps]

    give, own, *outgoing = call(
        functools.partial(spill_kernel, dp_count, room),
        [SM, HB, HB],
        [VM, VM] + [HB] * peers,
        [vmem((moved, own_rows), BF16), vmem((own_rows, width), BF16)] + [hbm((room, width), BF16)] * peers,
        [vmem((dp_count, own_rows), I32), vmem((moved, width), BF16), DMA(()), DMA((PIECES,)), DMA((PIECES * peers,))],
        2 * moved * own_rows * width,
        4 * own_rows * width,
        "spill_pick",
    )(me, in_hbm(spill_rows), own_in)
    arrived = shift(outgoing, 1)

    level_count = gate_table.shape[0]
    index_t = gate_index[0].T
    ids_t = expert_ids[0].T
    matches = index_t[:, None, :] == jnp.arange(level_count, dtype=I32)[None, :, None]
    picked = jnp.sum(jnp.where(matches, gate_table[None, :, None], 0.0), axis=1)
    weight = picked / jnp.sum(picked, axis=0, keepdims=True)
    pick, own_w, arr_w = call(
        functools.partial(route_kernel, dp_count, room, experts_all, capacity),
        [SM, VM, VM, VM],
        [VM] * 3,
        [vmem((slots, source_rows), BF16), vmem((2 * own_rows, slots), BF16), vmem((2 * moved, slots), BF16)],
        [],
        2 * column_tokens * column_tokens * 600,
        6 * slots * source_rows,
        "route",
    )(me, spill_rows, ids_t, weight)

    outbound = call(
        build_kernel,
        [VM] * (2 + peers),
        HB,
        hbm((slots, width), BF16),
        [vmem((slots, width), BF16), DMA((PIECES,))],
        2 * slots * source_rows * width,
        2 * (slots + source_rows) * width,
        "build",
    )(pick, own, *arrived)

    def exchange(rows):
        return lax.all_to_all(rows, "expert", split_axis=0, concat_axis=0, tiled=True)

    inbound = exchange(outbound.reshape(expert_count, capacity, width))
    tiles, downs = ff // GATE_COLS, width // DOWN_COLS
    outcome = call(
        ffn_kernel,
        [HB] * 4,
        HB,
        hbm((slots, width), BF16),
        [
            vmem((slots, width), BF16),
            vmem((tiles, width, 2 * GATE_COLS), BF16),
            vmem((downs, ff, DOWN_COLS), BF16),
            vmem((slots, 2 * GATE_COLS), F32),
            vmem((slots, ff), BF16),
            vmem((downs, slots, DOWN_COLS), BF16),
            DMA((PIECES,)),
            DMA((PIECES, 2)),
            DMA((tiles, 2)),
            DMA((downs,)),
            DMA((downs,)),
        ],
        6 * slots * width * ff,
        4 * slots * width + 6 * width * ff,
        "experts",
        FFN_GRANT,
    )(inbound.reshape(slots, width), w_gate[0], w_up[0], w_down[0])
    back = exchange(outcome.reshape(expert_count, capacity, width)).reshape(slots, width)

    arrived_parts = call(
        functools.partial(combine_arrived_kernel, room),
        [VM, HB],
        [HB] * peers,
        [hbm((room, width), BF16)] * peers,
        [vmem((slots, width), BF16), vmem((moved, width), BF16), DMA((PIECES,)), DMA((PIECES * peers,))],
        4 * moved * slots * width,
        2 * (slots + moved) * width,
        "combine_arrived",
    )(arr_w, in_hbm(back))
    returned = shift(arrived_parts, -1)
    own_part = call(
        combine_own_kernel,
        [VM, HB],
        VM,
        vmem((own_rows, width), F32),
        [vmem((slots, width), BF16), DMA((PIECES,))],
        4 * own_rows * slots * width,
        2 * slots * width + 4 * own_rows * width,
        "combine_own",
    )(own_w, in_hbm(back))
    mixed = call(
        finish_kernel,
        [VM] * (2 + peers),
        HB,
        hbm((own_rows, width), BF16),
        [vmem((own_rows, width), BF16), DMA((PIECES,))],
        2 * moved * own_rows * width,
        8 * own_rows * width,
        "finish",
    )(give, own_part, *returned)
    return mixed[None]


def solution(mesh):
    in_specs = (
        P("expert", "dp", None),
        P("expert", None, None),
        P("expert", None, None),
        P("expert", None, None),
        P("expert", None, None),
        P("expert", None, None),
        P(),
        P("expert", None),
    )
    out_specs = P("expert", "dp", None)
    return jax.shard_map(local, mesh=mesh, in_specs=in_specs, out_specs=out_specs, check_vma=False)
```

```python
import functools
import jax
import jax.numpy as jnp
from jax import lax
from jax.experimental import pallas as pl
from jax.experimental.pallas import tpu as pltpu
from jax.sharding import PartitionSpec as P

F32 = jnp.float32
BF16 = jnp.bfloat16
I32 = jnp.int32


def onehot(mask):
    return jnp.where(mask, 1.0, 0.0).astype(BF16)


def strict_upper(n):
    return onehot(lax.broadcasted_iota(I32, (n, n), 0) < lax.broadcasted_iota(I32, (n, n), 1))


def dot(a, b):
    return jnp.dot(a, b, preferred_element_type=F32)


def dot_nt(a, b):
    return lax.dot_general(a, b, (((1,), (1,)), ((), ())), preferred_element_type=F32)


def dot_tn(a, b):
    return lax.dot_general(a, b, (((0,), (0,)), ((), ())), preferred_element_type=F32)


def send(buf_ref, out_ref, sems, j):
    return pltpu.make_async_copy(buf_ref, out_ref, sems.at[j])


def parts(width, count):
    step = width // count
    return [pl.ds(j * step, step) for j in range(count)]


PIECES = 4


def spill_kernel(dp_count, room, me_ref, spill_ref, tok_ref, pick_ref, own_ref, *refs):
    out_refs, (spill_buf, buf, spill_sem, in_sems, out_sems) = refs[: dp_count - 1], refs[dp_count - 1 :]
    own_rows, width = tok_ref.shape
    slots = pick_ref.shape[0]
    load = pltpu.make_async_copy(spill_ref, spill_buf, spill_sem)
    load.start()
    cols = parts(width, PIECES)
    loads = [send(tok_ref.at[:, c], own_ref.at[:, c], in_sems, j) for j, c in enumerate(cols)]
    for copy in loads:
        copy.start()
    load.wait()
    me = me_ref[0]
    senders = spill_buf[pl.ds(me, 1), :]
    peers = lax.broadcasted_iota(I32, (8, own_rows), 0)
    same = onehot(senders == peers)
    before = dot(same, strict_upper(own_rows))
    order = jnp.sum(before * same.astype(F32), axis=0, keepdims=True).astype(I32)
    ahead = jnp.where(senders < me, senders - me + dp_count, senders - me)
    target = jnp.where(ahead == 0, slots, (ahead - 1) * room + order)
    rows = lax.broadcasted_iota(I32, (slots, own_rows), 0)
    pick = onehot(rows == target)
    pick_ref[...] = pick
    stores = []
    for j, c in enumerate(cols):
        loads[j].wait()
        buf[:, c] = dot(pick, own_ref[:, c]).astype(BF16)
        for k, out_ref in enumerate(out_refs):
            store = send(buf.at[pl.ds(k * room, room), c], out_ref.at[:, c], out_sems, j * len(out_refs) + k)
            store.start()
            stores.append(store)
    for store in stores:
        store.wait()


Z, Y, C = 4, 4, 2


def partner(me, k, sign):
    z = (me // (Y * C) + sign * (k // (Y * C))) % Z
    y = (me // C % Y + sign * (k // C % Y)) % Y
    c = (me % C + k % C) % C
    return (z * Y + y) * C + c


def slot_of(index, experts_all, capacity, first):
    cut = experts_all * first
    in_first = index < cut
    expert = jnp.where(in_first, index // first, (index - cut) // (capacity - first))
    rank = jnp.where(in_first, index % first, first + (index - cut) % (capacity - first))
    return expert, rank + 1


def route_kernel(
    dp_count, room, experts_all, capacity, first, me_ref, spill_ref, ids_ref, weight_ref,
    pick_ref, own_w_ref, arr_w_ref
):
    me = me_ref[0]
    own_rows = spill_ref.shape[1]
    top_count, column_tokens = ids_ref.shape
    source_rows = own_rows + (dp_count - 1) * room
    slots = experts_all * capacity

    by_home = onehot(spill_ref[...] == me)
    order = dot(by_home, strict_upper(own_rows)).astype(I32)
    homes = lax.broadcasted_iota(I32, (dp_count, own_rows), 0)
    place = lax.broadcasted_iota(I32, (dp_count, own_rows), 1)
    back = jnp.where(homes > me, me - homes + dp_count, me - homes)
    row = jnp.where(back == 0, place, own_rows + (back - 1) * room + order)
    row = jnp.where(spill_ref[...] == me, row, source_rows)
    row = jnp.concatenate([row[h : h + 1] for h in range(dp_count)], axis=1)
    to_row = onehot(lax.broadcasted_iota(I32, (source_rows, column_tokens), 0) == row)

    experts = lax.broadcasted_iota(I32, (experts_all, column_tokens), 0)
    scale = jnp.zeros((experts_all, column_tokens), F32)
    chosen = jnp.zeros((experts_all, column_tokens), F32)
    mine = row < source_rows
    for k in range(top_count):
        hit = (ids_ref[k : k + 1, :] == experts) & mine
        scale = jnp.where(hit, weight_ref[k : k + 1, :], scale)
        chosen = jnp.where(hit, 1.0, chosen)
    rank = dot(chosen.astype(BF16), strict_upper(column_tokens))
    keep = (chosen > 0.0) & (rank < capacity)
    code = jnp.where(keep, rank + 1.0, 0.0).astype(BF16)
    scale = jnp.where(keep, scale, 0.0)
    high = scale.astype(BF16)
    low = (scale - high.astype(F32)).astype(BF16)

    slot_expert, _ = slot_of(lax.broadcasted_iota(I32, (slots, experts_all), 0), experts_all, capacity, first)
    slot_row = lax.broadcasted_iota(I32, (slots, experts_all), 0)
    slot_expert = jnp.where(slot_row < experts_all * first, slot_expert, partner(me_ref[1], slot_expert, 1))
    spread = onehot(slot_expert == lax.broadcasted_iota(I32, (slots, experts_all), 1))
    code_rows = dot_nt(code, to_row).astype(BF16)
    _, rank_col = slot_of(lax.broadcasted_iota(I32, (slots, source_rows), 0), experts_all, capacity, first)
    pick_ref[...] = onehot(dot(spread, code_rows).astype(I32) == rank_col)

    slot_expert, _ = slot_of(lax.broadcasted_iota(I32, (experts_all, slots), 1), experts_all, capacity, first)
    spread_t = onehot(slot_expert == lax.broadcasted_iota(I32, (experts_all, slots), 0))
    _, rank_row = slot_of(lax.broadcasted_iota(I32, (source_rows, slots), 1), experts_all, capacity, first)
    code_t = dot_nt(to_row, code).astype(BF16)
    filled = dot(code_t, spread_t).astype(I32) == rank_row
    high_t = dot(dot_nt(to_row, high).astype(BF16), spread_t)
    low_t = dot(dot_nt(to_row, low).astype(BF16), spread_t)
    high_w = jnp.where(filled, high_t, 0.0).astype(BF16)
    low_w = jnp.where(filled, low_t, 0.0).astype(BF16)
    own_w_ref[:own_rows] = high_w[:own_rows]
    own_w_ref[own_rows:] = low_w[:own_rows]
    arr_w_ref[: source_rows - own_rows] = high_w[own_rows:]
    arr_w_ref[source_rows - own_rows :] = low_w[own_rows:]


def build_kernel(pick_ref, *refs):
    *src_refs, out_ref, buf, sems = refs
    copies = []
    for j, c in enumerate(parts(out_ref.shape[1], PIECES)):
        rows = jnp.concatenate([ref[:, c] for ref in src_refs], axis=0)
        buf[:, c] = dot(pick_ref[...], rows).astype(BF16)
        copies.append(send(buf.at[:, c], out_ref.at[:, c], sems, j))
        copies[-1].start()
    for copy in copies:
        copy.wait()


def build_blocks_kernel(size, pick_ref, *refs):
    count = pick_ref.shape[0] // size
    src_refs, out_refs, (buf, sems) = refs[: -count - 2], refs[-count - 2 : -2], refs[-2:]
    for c in parts(buf.shape[1], PIECES):
        rows = jnp.concatenate([ref[:, c] for ref in src_refs], axis=0)
        buf[:, c] = dot(pick_ref[...], rows).astype(BF16)
    copies = [send(buf.at[pl.ds(k * size, size)], out_ref, sems, k) for k, out_ref in enumerate(out_refs)]
    for copy in copies:
        copy.start()
    for copy in copies:
        copy.wait()


GATE_COLS = 128
DOWN_COLS = 1024


def ffn_kernel(blocks, me_ref, *refs):
    x_in, (gate_in, up_in, down_in, out_ref, x, both, down, acc, hidden, buf) = refs[:blocks], refs[blocks : blocks + 10]
    x_sem, top_sem, both_sem, down_sem, out_sem = refs[blocks + 10 :]
    depth = x.shape[1] // PIECES
    tiles, downs = both.shape[0], down.shape[0]
    size = x.shape[0] // blocks

    def lanes(n, step):
        return pl.ds(pl.multiple_of(n * step, step), step)

    def fetch(n):
        cols = lanes(n, GATE_COLS)
        return (
            pltpu.make_async_copy(gate_in.at[:, cols], both.at[n, :, pl.ds(0, GATE_COLS)], both_sem.at[n, 0]),
            pltpu.make_async_copy(up_in.at[:, cols], both.at[n, :, pl.ds(GATE_COLS, GATE_COLS)], both_sem.at[n, 1]),
        )

    def fetch_down(n):
        return pltpu.make_async_copy(down_in.at[:, lanes(n, DOWN_COLS)], down.at[n], down_sem.at[n])

    def store(n):
        cols = lanes(n, DOWN_COLS)
        return pltpu.make_async_copy(buf.at[:, cols], out_ref.at[:, cols], out_sem.at[n])

    def activate(n):
        gate_part, up_part = acc[:, :GATE_COLS], acc[:, GATE_COLS:]
        hidden[:, lanes(n, GATE_COLS)] = (jax.nn.silu(gate_part) * up_part).astype(BF16)

    def top(k):
        d = lanes(k, depth)
        rows = [] if blocks > 1 else [pltpu.make_async_copy(x_in[0].at[:, d], x.at[:, d], x_sem.at[k])]
        return rows + [
            pltpu.make_async_copy(gate_in.at[d, pl.ds(0, GATE_COLS)], both.at[0, d, pl.ds(0, GATE_COLS)], top_sem.at[k, 0]),
            pltpu.make_async_copy(up_in.at[d, pl.ds(0, GATE_COLS)], both.at[0, d, pl.ds(GATE_COLS, GATE_COLS)], top_sem.at[k, 1]),
        ]

    whole = []
    if blocks > 1:
        whole = [send(x_in[k], x.at[pl.ds(k * size, size)], x_sem, k) for k in range(blocks)]
    for copy in whole:
        copy.start()
    for k in range(PIECES):
        for copy in top(k):
            copy.start()
    for copy in whole:
        copy.wait()
    acc[...] = jnp.zeros_like(acc)

    @pl.loop(0, PIECES)
    def _(k):
        for copy in top(k):
            copy.wait()
        for ahead in (1, 2):

            @pl.when(k == 2 * ahead - 1)
            def _():
                for copy in fetch(ahead):
                    copy.start()

        d = lanes(k, depth)
        acc[...] += dot(x[:, d], both[0, d, :])

    activate(0)

    @pl.loop(1, tiles)
    def _(n):
        for copy in fetch(n):
            copy.wait()

        @pl.when(n + 2 < tiles)
        def _():
            for copy in fetch(n + 2):
                copy.start()

        @pl.when(n + 2 >= tiles)
        def _():
            half = (n + 2 - tiles) * (downs // 2)
            for j in range(downs // 2):
                fetch_down(half + j).start()

        acc[...] = dot(x[...], both[n])
        activate(n)

    @pl.loop(0, downs)
    def _(n):
        fetch_down(n).wait()
        buf[:, lanes(n, DOWN_COLS)] = dot(hidden[...], down[n]).astype(BF16)
        if blocks == 1:
            store(n).start()

    if blocks == 1:

        @pl.loop(0, downs)
        def _(n):
            store(n).wait()

    else:
        stores = []
        for k in range(blocks):
            home = partner(me_ref[1], k, -1)
            stores.append(send(buf.at[pl.ds(k * size, size)], out_ref.at[home], out_sem, k))
            stores[-1].start()
        for copy in stores:
            copy.wait()


def weighted(w_ref, res):
    both = dot(w_ref[...], res)
    half = both.shape[0] // 2
    return both[:half] + both[half:]


def each_piece(res_ref, res, sems):
    cols = parts(res.shape[1], PIECES)
    loads = [send(res_ref.at[:, c], res.at[:, c], sems, j) for j, c in enumerate(cols)]
    for load in loads:
        load.start()
    for j, c in enumerate(cols):
        loads[j].wait()
        yield j, c


def combine_first_kernel(own_w_ref, arr_w_ref, res_ref, own_ref, arr_ref, res, own_buf, arr_buf, in_sems, sems):
    copies = []
    for j, c in each_piece(res_ref, res, in_sems):
        own_buf[:, c] = weighted(own_w_ref, res[:, c])
        arr_buf[:, c] = weighted(arr_w_ref, res[:, c])
        copies.append(send(own_buf.at[:, c], own_ref.at[:, c], sems, 2 * j))
        copies.append(send(arr_buf.at[:, c], arr_ref.at[:, c], sems, 2 * j + 1))
        copies[-2].start()
        copies[-1].start()
    for copy in copies:
        copy.wait()


def with_part(res_ref, part_ref, res, part, in_sems, part_sems):
    cols = parts(res.shape[1], PIECES)
    loads = [send(part_ref.at[:, c], part.at[:, c], part_sems, j) for j, c in enumerate(cols)]
    for load in loads:
        load.start()
    for j, c in each_piece(res_ref, res, in_sems):
        loads[j].wait()
        yield j, c


def combine_own_kernel(w_ref, res_ref, part_ref, out_ref, res, part, in_sems, part_sems):
    for _, c in with_part(res_ref, part_ref, res, part, in_sems, part_sems):
        out_ref[:, c] = part[:, c] + weighted(w_ref, res[:, c])


def combine_arrived_kernel(room, w_ref, res_ref, part_ref, *refs):
    *out_refs, res, part, buf, in_sems, part_sems, sems = refs
    copies = []
    for j, c in with_part(res_ref, part_ref, res, part, in_sems, part_sems):
        buf[:, c] = (part[:, c] + weighted(w_ref, res[:, c])).astype(BF16)
        for k, out_ref in enumerate(out_refs):
            copies.append(send(buf.at[pl.ds(k * room, room), c], out_ref.at[:, c], sems, j * len(out_refs) + k))
            copies[-1].start()
    for copy in copies:
        copy.wait()


def finish_kernel(pick_ref, own_ref, *refs):
    *back_refs, out_ref, buf, sems = refs
    copies = []
    for j, c in enumerate(parts(out_ref.shape[1], PIECES)):
        back = jnp.concatenate([ref[:, c] for ref in back_refs], axis=0)
        buf[:, c] = (own_ref[:, c] + dot_tn(pick_ref[...], back)).astype(BF16)
        copies.append(send(buf.at[:, c], out_ref.at[:, c], sems, j))
        copies[-1].start()
    for copy in copies:
        copy.wait()


GRANT = 24 * 1024 * 1024
FFN_GRANT = 56 * 1024 * 1024


def in_hbm(x):
    return pltpu.with_memory_space_constraint(x, pltpu.HBM)


VM = pl.BlockSpec(memory_space=pltpu.VMEM)
SM = pl.BlockSpec(memory_space=pltpu.SMEM)
HB = pl.BlockSpec(memory_space=pltpu.HBM)
DMA = pltpu.SemaphoreType.DMA


def call(kernel, in_specs, out_specs, out_shape, scratch, flops, size, grant=GRANT):
    return pl.pallas_call(
        kernel,
        in_specs=in_specs,
        out_specs=out_specs,
        out_shape=out_shape,
        scratch_shapes=scratch,
        compiler_params=pltpu.CompilerParams(vmem_limit_bytes=grant),
        cost_estimate=pl.CostEstimate(flops=flops, bytes_accessed=size, transcendentals=0),
    )


def local(tokens, w_gate, w_up, w_down, expert_ids, gate_index, gate_table, spill):
    dp_count = lax.axis_size("dp")
    expert_count = lax.axis_size("expert")
    own_rows, width = tokens.shape[1:]
    column_tokens = spill.shape[1]
    top_count = expert_ids.shape[2]
    experts_all = w_gate.shape[0] * expert_count
    capacity = 3 * own_rows * top_count // (2 * experts_all)
    room = own_rows // 4
    moved = (dp_count - 1) * room
    source_rows = own_rows + moved
    slots = experts_all * capacity
    ff = w_gate.shape[2]
    first = capacity - 8
    cut = experts_all * first
    rest = slots - cut
    me = jnp.stack([lax.axis_index("dp"), lax.axis_index("expert")]).astype(I32)
    own_in = in_hbm(tokens[0])
    spill_rows = spill.reshape(dp_count, own_rows)
    hbm, vmem = pltpu.HBM, pltpu.VMEM
    steps = range(1, dp_count)
    peers = len(steps)

    def shift(blocks, sign):
        sent = {}
        for k in sorted(steps, key=lambda k: abs(dp_count - 2 * k)):
            pairs = [(i, (i + sign * k) % dp_count) for i in range(dp_count)]
            sent[k] = lax.ppermute(blocks[k - 1], "dp", pairs)
        return [sent[k] for k in steps]

    give, own, *outgoing = call(
        functools.partial(spill_kernel, dp_count, room),
        [SM, HB, HB],
        [VM, VM] + [HB] * peers,
        [vmem((moved, own_rows), BF16), vmem((own_rows, width), BF16)] + [hbm((room, width), BF16)] * peers,
        [vmem((dp_count, own_rows), I32), vmem((moved, width), BF16), DMA(()), DMA((PIECES,)), DMA((PIECES * peers,))],
        2 * moved * own_rows * width,
        4 * own_rows * width,
    )(me, in_hbm(spill_rows), own_in)
    arrived = shift(outgoing, 1)

    level_count = gate_table.shape[0]
    index_t = gate_index[0].T
    ids_t = expert_ids[0].T
    matches = index_t[:, None, :] == jnp.arange(level_count, dtype=I32)[None, :, None]
    picked = jnp.sum(jnp.where(matches, gate_table[None, :, None], 0.0), axis=1)
    weight = picked / jnp.sum(picked, axis=0, keepdims=True)
    pick, own_w, arr_w = call(
        functools.partial(route_kernel, dp_count, room, experts_all, capacity, first),
        [SM, VM, VM, VM],
        [VM] * 3,
        [vmem((slots, source_rows), BF16), vmem((2 * own_rows, slots), BF16), vmem((2 * moved, slots), BF16)],
        [],
        2 * column_tokens * column_tokens * 600,
        6 * slots * source_rows,
    )(me, spill_rows, ids_t, weight)

    def exchange(rows):
        shaped = rows.reshape(expert_count, -1, width)
        return lax.all_to_all(shaped, "expert", split_axis=0, concat_axis=0, tiled=True).reshape(-1, width)

    outbound = call(
        build_kernel,
        [VM] * (2 + peers),
        HB,
        hbm((cut, width), BF16),
        [vmem((cut, width), BF16), DMA((PIECES,))],
        2 * cut * source_rows * width,
        2 * (cut + source_rows) * width,
    )(pick[:cut], own, *arrived)
    inbound = exchange(outbound)
    size = rest // expert_count
    blocks = call(
        functools.partial(build_blocks_kernel, size),
        [VM] * (2 + peers),
        [HB] * expert_count,
        [hbm((size, width), BF16)] * expert_count,
        [vmem((rest, width), BF16), DMA((expert_count,))],
        2 * rest * source_rows * width,
        2 * (rest + source_rows) * width,
    )(pick[cut:], own, *arrived)

    def far(k):
        z, y = k // (Y * C), k // C % Y
        return -(min(z, Z - z) + min(y, Y - y))

    landed = {0: blocks[0]}
    for k in sorted(range(1, expert_count), key=far):
        landed[k] = lax.ppermute(blocks[k], "expert", [(i, partner(i, k, 1)) for i in range(expert_count)])

    tiles, downs = ff // GATE_COLS, width // DOWN_COLS

    def experts(inputs, count, out_shape):
        blocks = len(inputs)
        return call(
            functools.partial(ffn_kernel, blocks),
            [SM] + [HB] * (blocks + 3),
            HB,
            hbm(out_shape, BF16),
            [
                vmem((count, width), BF16),
                vmem((tiles, width, 2 * GATE_COLS), BF16),
                vmem((downs, ff, DOWN_COLS), BF16),
                vmem((count, 2 * GATE_COLS), F32),
                vmem((count, ff), BF16),
                vmem((count, width), BF16),
                DMA((max(blocks, PIECES),)),
                DMA((PIECES, 2)),
                DMA((tiles, 2)),
                DMA((downs,)),
                DMA((max(blocks, downs),)),
            ],
            6 * count * width * ff,
            4 * count * width + 6 * width * ff,
            FFN_GRANT,
        )(me, *inputs, w_gate[0], w_up[0], w_down[0])

    outcome = experts([inbound], cut, (cut, width))
    back0 = exchange(outcome)
    arrivals = [in_hbm(landed[k]) for k in range(expert_count)]
    back1 = exchange(experts(arrivals, rest, (expert_count, size, width)))

    part_own, part_arr = call(
        combine_first_kernel,
        [VM, VM, HB],
        [HB] * 2,
        [hbm((own_rows, width), F32), hbm((moved, width), F32)],
        [
            vmem((cut, width), BF16),
            vmem((own_rows, width), F32),
            vmem((moved, width), F32),
            DMA((PIECES,)),
            DMA((2 * PIECES,)),
        ],
        4 * source_rows * cut * width,
        2 * cut * width + 4 * source_rows * width,
    )(own_w[:, :cut], arr_w[:, :cut], in_hbm(back0))
    back1 = in_hbm(back1)
    arrived_parts = call(
        functools.partial(combine_arrived_kernel, room),
        [VM, HB, HB],
        [HB] * peers,
        [hbm((room, width), BF16)] * peers,
        [
            vmem((rest, width), BF16),
            vmem((moved, width), F32),
            vmem((moved, width), BF16),
            DMA((PIECES,)),
            DMA((PIECES,)),
            DMA((PIECES * peers,)),
        ],
        4 * moved * rest * width,
        2 * rest * width + 6 * moved * width,
    )(arr_w[:, cut:], back1, in_hbm(part_arr))
    returned = shift(arrived_parts, -1)
    own_part = call(
        combine_own_kernel,
        [VM, HB, HB],
        VM,
        vmem((own_rows, width), F32),
        [vmem((rest, width), BF16), vmem((own_rows, width), F32), DMA((PIECES,)), DMA((PIECES,))],
        4 * own_rows * rest * width,
        2 * rest * width + 8 * own_rows * width,
    )(own_w[:, cut:], back1, in_hbm(part_own))
    mixed = call(
        finish_kernel,
        [VM] * (2 + peers),
        HB,
        hbm((own_rows, width), BF16),
        [vmem((own_rows, width), BF16), DMA((PIECES,))],
        2 * moved * own_rows * width,
        8 * own_rows * width,
    )(give, own_part, *returned)
    return mixed[None]


def solution(mesh):
    in_specs = (
        P("expert", "dp", None),
        P("expert", None, None),
        P("expert", None, None),
        P("expert", None, None),
        P("expert", None, None),
        P("expert", None, None),
        P(),
        P("expert", None),
    )
    out_specs = P("expert", "dp", None)

    return jax.shard_map(local, mesh=mesh, in_specs=in_specs, out_specs=out_specs, check_vma=False)
```

```python
import functools
import jax
import jax.numpy as jnp
from jax import lax
from jax.experimental import pallas as pl
from jax.experimental.pallas import tpu as pltpu
from jax.sharding import PartitionSpec as P

F32 = jnp.float32
BF16 = jnp.bfloat16
I32 = jnp.int32


def onehot(mask):
    return jnp.where(mask, 1.0, 0.0).astype(BF16)


def strict_upper(n):
    return onehot(lax.broadcasted_iota(I32, (n, n), 0) < lax.broadcasted_iota(I32, (n, n), 1))


def dot(a, b):
    return jnp.dot(a, b, preferred_element_type=F32)


def dot_nt(a, b):
    return lax.dot_general(a, b, (((1,), (1,)), ((), ())), preferred_element_type=F32)


def dot_tn(a, b):
    return lax.dot_general(a, b, (((0,), (0,)), ((), ())), preferred_element_type=F32)


def send(buf_ref, out_ref, sems, j):
    return pltpu.make_async_copy(buf_ref, out_ref, sems.at[j])


def parts(width, count):
    step = width // count
    return [pl.ds(j * step, step) for j in range(count)]


PIECES = 4


def spill_kernel(dp_count, room, me_ref, spill_ref, tok_ref, pick_ref, own_ref, *refs):
    out_refs, (spill_buf, buf, spill_sem, in_sems, out_sems) = refs[: dp_count - 1], refs[dp_count - 1 :]
    own_rows, width = tok_ref.shape
    slots = pick_ref.shape[0]
    load = pltpu.make_async_copy(spill_ref, spill_buf, spill_sem)
    load.start()
    cols = parts(width, PIECES)
    loads = [send(tok_ref.at[:, c], own_ref.at[:, c], in_sems, j) for j, c in enumerate(cols)]
    for copy in loads:
        copy.start()
    load.wait()
    me = me_ref[0]
    senders = spill_buf[pl.ds(me, 1), :]
    peers = lax.broadcasted_iota(I32, (8, own_rows), 0)
    same = onehot(senders == peers)
    before = dot(same, strict_upper(own_rows))
    order = jnp.sum(before * same.astype(F32), axis=0, keepdims=True).astype(I32)
    ahead = jnp.where(senders < me, senders - me + dp_count, senders - me)
    target = jnp.where(ahead == 0, slots, (ahead - 1) * room + order)
    rows = lax.broadcasted_iota(I32, (slots, own_rows), 0)
    pick = onehot(rows == target)
    pick_ref[...] = pick
    stores = []
    for j, c in enumerate(cols):
        loads[j].wait()
        buf[:, c] = dot(pick, own_ref[:, c]).astype(BF16)
        for k, out_ref in enumerate(out_refs):
            store = send(buf.at[pl.ds(k * room, room), c], out_ref.at[:, c], out_sems, j * len(out_refs) + k)
            store.start()
            stores.append(store)
    for store in stores:
        store.wait()


Z, Y, C = 4, 4, 2


def partner(me, k, sign):
    z = (me // (Y * C) + sign * (k // (Y * C))) % Z
    y = (me // C % Y + sign * (k // C % Y)) % Y
    c = (me % C + k % C) % C
    return (z * Y + y) * C + c


def slot_of(index, experts_all, capacity, first):
    cut = experts_all * first
    in_first = index < cut
    expert = jnp.where(in_first, index // first, (index - cut) // (capacity - first))
    rank = jnp.where(in_first, index % first, first + (index - cut) % (capacity - first))
    return expert, rank + 1


def route_kernel(
    dp_count, room, experts_all, capacity, first, me_ref, spill_ref, ids_ref, weight_ref,
    pick_ref, own_w_ref, arr_w_ref
):
    me = me_ref[0]
    own_rows = spill_ref.shape[1]
    top_count, column_tokens = ids_ref.shape
    source_rows = own_rows + (dp_count - 1) * room
    slots = experts_all * capacity

    by_home = onehot(spill_ref[...] == me)
    order = dot(by_home, strict_upper(own_rows)).astype(I32)
    homes = lax.broadcasted_iota(I32, (dp_count, own_rows), 0)
    place = lax.broadcasted_iota(I32, (dp_count, own_rows), 1)
    back = jnp.where(homes > me, me - homes + dp_count, me - homes)
    row = jnp.where(back == 0, place, own_rows + (back - 1) * room + order)
    row = jnp.where(spill_ref[...] == me, row, source_rows)
    row = jnp.concatenate([row[h : h + 1] for h in range(dp_count)], axis=1)
    to_row = onehot(lax.broadcasted_iota(I32, (source_rows, column_tokens), 0) == row)

    experts = lax.broadcasted_iota(I32, (experts_all, column_tokens), 0)
    scale = jnp.zeros((experts_all, column_tokens), F32)
    chosen = jnp.zeros((experts_all, column_tokens), F32)
    mine = row < source_rows
    for k in range(top_count):
        hit = (ids_ref[k : k + 1, :] == experts) & mine
        scale = jnp.where(hit, weight_ref[k : k + 1, :], scale)
        chosen = jnp.where(hit, 1.0, chosen)
    rank = dot(chosen.astype(BF16), strict_upper(column_tokens))
    keep = (chosen > 0.0) & (rank < capacity)
    code = jnp.where(keep, rank + 1.0, 0.0).astype(BF16)
    scale = jnp.where(keep, scale, 0.0)
    high = scale.astype(BF16)
    low = (scale - high.astype(F32)).astype(BF16)

    slot_expert, _ = slot_of(lax.broadcasted_iota(I32, (slots, experts_all), 0), experts_all, capacity, first)
    slot_row = lax.broadcasted_iota(I32, (slots, experts_all), 0)
    slot_expert = jnp.where(slot_row < experts_all * first, slot_expert, partner(me_ref[1], slot_expert, 1))
    spread = onehot(slot_expert == lax.broadcasted_iota(I32, (slots, experts_all), 1))
    code_rows = dot_nt(code, to_row).astype(BF16)
    _, rank_col = slot_of(lax.broadcasted_iota(I32, (slots, source_rows), 0), experts_all, capacity, first)
    pick_ref[...] = onehot(dot(spread, code_rows).astype(I32) == rank_col)

    slot_expert, _ = slot_of(lax.broadcasted_iota(I32, (experts_all, slots), 1), experts_all, capacity, first)
    spread_t = onehot(slot_expert == lax.broadcasted_iota(I32, (experts_all, slots), 0))
    _, rank_row = slot_of(lax.broadcasted_iota(I32, (source_rows, slots), 1), experts_all, capacity, first)
    code_t = dot_nt(to_row, code).astype(BF16)
    filled = dot(code_t, spread_t).astype(I32) == rank_row
    high_t = dot(dot_nt(to_row, high).astype(BF16), spread_t)
    low_t = dot(dot_nt(to_row, low).astype(BF16), spread_t)
    high_w = jnp.where(filled, high_t, 0.0).astype(BF16)
    low_w = jnp.where(filled, low_t, 0.0).astype(BF16)
    own_w_ref[:own_rows] = high_w[:own_rows]
    own_w_ref[own_rows:] = low_w[:own_rows]
    arr_w_ref[: source_rows - own_rows] = high_w[own_rows:]
    arr_w_ref[source_rows - own_rows :] = low_w[own_rows:]


def build_kernel(pick_ref, *refs):
    *src_refs, out_ref, buf, sems = refs
    copies = []
    for j, c in enumerate(parts(out_ref.shape[1], PIECES)):
        rows = jnp.concatenate([ref[:, c] for ref in src_refs], axis=0)
        buf[:, c] = dot(pick_ref[...], rows).astype(BF16)
        copies.append(send(buf.at[:, c], out_ref.at[:, c], sems, j))
        copies[-1].start()
    for copy in copies:
        copy.wait()


def build_blocks_kernel(size, pick_ref, *refs):
    count = pick_ref.shape[0] // size
    src_refs, out_refs, (buf, sems) = refs[: -count - 2], refs[-count - 2 : -2], refs[-2:]
    for c in parts(buf.shape[1], PIECES):
        rows = jnp.concatenate([ref[:, c] for ref in src_refs], axis=0)
        buf[:, c] = dot(pick_ref[...], rows).astype(BF16)
    copies = [send(buf.at[pl.ds(k * size, size)], out_ref, sems, k) for k, out_ref in enumerate(out_refs)]
    for copy in copies:
        copy.start()
    for copy in copies:
        copy.wait()


def regroup_kernel(size, *refs):
    *in_refs, out_ref, buf, in_sems, out_sem = refs
    loads = [send(ref.at[pl.ds(size, size)], buf.at[pl.ds(j * size, size)], in_sems, j) for j, ref in enumerate(in_refs)]
    for load in loads:
        load.start()
    for load in loads:
        load.wait()
    store = send(buf, out_ref, out_sem, 0)
    store.start()
    store.wait()


GATE_COLS = 128
DOWN_COLS = 1024


def ffn_kernel(blocks, inputs, me_ref, *refs):
    x_in, (gate_in, up_in, down_in, out_ref, x, both, down, acc, hidden, buf) = refs[:inputs], refs[inputs : inputs + 10]
    x_sem, top_sem, both_sem, down_sem, out_sem = refs[inputs + 10 :]
    depth = x.shape[1] // PIECES
    tiles, downs = both.shape[0], down.shape[0]
    size = x.shape[0] // blocks

    def lanes(n, step):
        return pl.ds(pl.multiple_of(n * step, step), step)

    def fetch(n):
        cols = lanes(n, GATE_COLS)
        return (
            pltpu.make_async_copy(gate_in.at[:, cols], both.at[n, :, pl.ds(0, GATE_COLS)], both_sem.at[n, 0]),
            pltpu.make_async_copy(up_in.at[:, cols], both.at[n, :, pl.ds(GATE_COLS, GATE_COLS)], both_sem.at[n, 1]),
        )

    def fetch_down(n):
        return pltpu.make_async_copy(down_in.at[:, lanes(n, DOWN_COLS)], down.at[n], down_sem.at[n])

    def store(n):
        cols = lanes(n, DOWN_COLS)
        return pltpu.make_async_copy(buf.at[:, cols], out_ref.at[:, cols], out_sem.at[n])

    def activate(n):
        gate_part, up_part = acc[:, :GATE_COLS], acc[:, GATE_COLS:]
        hidden[:, lanes(n, GATE_COLS)] = (jax.nn.silu(gate_part) * up_part).astype(BF16)

    def top(k):
        d = lanes(k, depth)
        rows = [] if blocks > 1 else [pltpu.make_async_copy(x_in[0].at[:, d], x.at[:, d], x_sem.at[k])]
        return rows + [
            pltpu.make_async_copy(gate_in.at[d, pl.ds(0, GATE_COLS)], both.at[0, d, pl.ds(0, GATE_COLS)], top_sem.at[k, 0]),
            pltpu.make_async_copy(up_in.at[d, pl.ds(0, GATE_COLS)], both.at[0, d, pl.ds(GATE_COLS, GATE_COLS)], top_sem.at[k, 1]),
        ]

    whole = []
    if blocks > 1:
        for k in range(blocks):
            chip, core = k // C, k % C
            ref, row = (x_in[-1], chip * size) if core else (x_in[chip], 0)
            whole.append(send(ref.at[pl.ds(row, size)], x.at[pl.ds(k * size, size)], x_sem, k))
    for copy in whole:
        copy.start()
    for k in range(PIECES):
        for copy in top(k):
            copy.start()
    for copy in whole:
        copy.wait()
    acc[...] = jnp.zeros_like(acc)

    @pl.loop(0, PIECES)
    def _(k):
        for copy in top(k):
            copy.wait()
        for ahead in (1, 2):

            @pl.when(k == 2 * ahead - 1)
            def _():
                for copy in fetch(ahead):
                    copy.start()

        d = lanes(k, depth)
        acc[...] += dot(x[:, d], both[0, d, :])

    activate(0)

    @pl.loop(1, tiles)
    def _(n):
        for copy in fetch(n):
            copy.wait()

        @pl.when(n + 2 < tiles)
        def _():
            for copy in fetch(n + 2):
                copy.start()

        @pl.when(n + 2 >= tiles)
        def _():
            half = (n + 2 - tiles) * (downs // 2)
            for j in range(downs // 2):
                fetch_down(half + j).start()

        acc[...] = dot(x[...], both[n])
        activate(n)

    @pl.loop(0, downs)
    def _(n):
        fetch_down(n).wait()
        buf[:, lanes(n, DOWN_COLS)] = dot(hidden[...], down[n]).astype(BF16)
        if blocks == 1:
            store(n).start()

    if blocks == 1:

        @pl.loop(0, downs)
        def _(n):
            store(n).wait()

    else:
        stores = []
        for k in range(blocks):
            home = partner(me_ref[1], k, -1)
            stores.append(send(buf.at[pl.ds(k * size, size)], out_ref.at[home], out_sem, k))
            stores[-1].start()
        for copy in stores:
            copy.wait()


def weighted(w_ref, res):
    both = dot(w_ref[...], res)
    half = both.shape[0] // 2
    return both[:half] + both[half:]


def each_piece(res_ref, res, sems):
    cols = parts(res.shape[1], PIECES)
    loads = [send(res_ref.at[:, c], res.at[:, c], sems, j) for j, c in enumerate(cols)]
    for load in loads:
        load.start()
    for j, c in enumerate(cols):
        loads[j].wait()
        yield j, c


def combine_first_kernel(own_w_ref, arr_w_ref, res_ref, own_ref, arr_ref, res, own_buf, arr_buf, in_sems, sems):
    copies = []
    for j, c in each_piece(res_ref, res, in_sems):
        own_buf[:, c] = weighted(own_w_ref, res[:, c])
        arr_buf[:, c] = weighted(arr_w_ref, res[:, c])
        copies.append(send(own_buf.at[:, c], own_ref.at[:, c], sems, 2 * j))
        copies.append(send(arr_buf.at[:, c], arr_ref.at[:, c], sems, 2 * j + 1))
        copies[-2].start()
        copies[-1].start()
    for copy in copies:
        copy.wait()


def with_part(res_ref, part_ref, res, part, in_sems, part_sems):
    cols = parts(res.shape[1], PIECES)
    loads = [send(part_ref.at[:, c], part.at[:, c], part_sems, j) for j, c in enumerate(cols)]
    for load in loads:
        load.start()
    for j, c in each_piece(res_ref, res, in_sems):
        loads[j].wait()
        yield j, c


def combine_own_kernel(w_ref, res_ref, part_ref, out_ref, res, part, in_sems, part_sems):
    for _, c in with_part(res_ref, part_ref, res, part, in_sems, part_sems):
        out_ref[:, c] = part[:, c] + weighted(w_ref, res[:, c])


def combine_arrived_kernel(room, w_ref, res_ref, part_ref, *refs):
    *out_refs, res, part, buf, in_sems, part_sems, sems = refs
    copies = []
    for j, c in with_part(res_ref, part_ref, res, part, in_sems, part_sems):
        buf[:, c] = (part[:, c] + weighted(w_ref, res[:, c])).astype(BF16)
        for k, out_ref in enumerate(out_refs):
            copies.append(send(buf.at[pl.ds(k * room, room), c], out_ref.at[:, c], sems, j * len(out_refs) + k))
            copies[-1].start()
    for copy in copies:
        copy.wait()


def finish_kernel(pick_ref, own_ref, *refs):
    *back_refs, out_ref, buf, sems = refs
    copies = []
    for j, c in enumerate(parts(out_ref.shape[1], PIECES)):
        back = jnp.concatenate([ref[:, c] for ref in back_refs], axis=0)
        buf[:, c] = (own_ref[:, c] + dot_tn(pick_ref[...], back)).astype(BF16)
        copies.append(send(buf.at[:, c], out_ref.at[:, c], sems, j))
        copies[-1].start()
    for copy in copies:
        copy.wait()


GRANT = 24 * 1024 * 1024
FFN_GRANT = 56 * 1024 * 1024


def in_hbm(x):
    return pltpu.with_memory_space_constraint(x, pltpu.HBM)


VM = pl.BlockSpec(memory_space=pltpu.VMEM)
SM = pl.BlockSpec(memory_space=pltpu.SMEM)
HB = pl.BlockSpec(memory_space=pltpu.HBM)
DMA = pltpu.SemaphoreType.DMA


def call(kernel, in_specs, out_specs, out_shape, scratch, flops, size, grant=GRANT):
    return pl.pallas_call(
        kernel,
        in_specs=in_specs,
        out_specs=out_specs,
        out_shape=out_shape,
        scratch_shapes=scratch,
        compiler_params=pltpu.CompilerParams(vmem_limit_bytes=grant),
        cost_estimate=pl.CostEstimate(flops=flops, bytes_accessed=size, transcendentals=0),
    )


def local(tokens, w_gate, w_up, w_down, expert_ids, gate_index, gate_table, spill):
    dp_count = lax.axis_size("dp")
    expert_count = lax.axis_size("expert")
    own_rows, width = tokens.shape[1:]
    column_tokens = spill.shape[1]
    top_count = expert_ids.shape[2]
    experts_all = w_gate.shape[0] * expert_count
    capacity = 3 * own_rows * top_count // (2 * experts_all)
    room = own_rows // 4
    moved = (dp_count - 1) * room
    source_rows = own_rows + moved
    slots = experts_all * capacity
    ff = w_gate.shape[2]
    first = capacity - 8
    cut = experts_all * first
    rest = slots - cut
    me = jnp.stack([lax.axis_index("dp"), lax.axis_index("expert")]).astype(I32)
    own_in = in_hbm(tokens[0])
    spill_rows = spill.reshape(dp_count, own_rows)
    hbm, vmem = pltpu.HBM, pltpu.VMEM
    steps = range(1, dp_count)
    peers = len(steps)

    def shift(blocks, sign):
        sent = {}
        for k in sorted(steps, key=lambda k: abs(dp_count - 2 * k)):
            pairs = [(i, (i + sign * k) % dp_count) for i in range(dp_count)]
            sent[k] = lax.ppermute(blocks[k - 1], "dp", pairs)
        return [sent[k] for k in steps]

    give, own, *outgoing = call(
        functools.partial(spill_kernel, dp_count, room),
        [SM, HB, HB],
        [VM, VM] + [HB] * peers,
        [vmem((moved, own_rows), BF16), vmem((own_rows, width), BF16)] + [hbm((room, width), BF16)] * peers,
        [vmem((dp_count, own_rows), I32), vmem((moved, width), BF16), DMA(()), DMA((PIECES,)), DMA((PIECES * peers,))],
        2 * moved * own_rows * width,
        4 * own_rows * width,
    )(me, in_hbm(spill_rows), own_in)
    arrived = shift(outgoing, 1)

    level_count = gate_table.shape[0]
    index_t = gate_index[0].T
    ids_t = expert_ids[0].T
    matches = index_t[:, None, :] == jnp.arange(level_count, dtype=I32)[None, :, None]
    picked = jnp.sum(jnp.where(matches, gate_table[None, :, None], 0.0), axis=1)
    weight = picked / jnp.sum(picked, axis=0, keepdims=True)
    pick, own_w, arr_w = call(
        functools.partial(route_kernel, dp_count, room, experts_all, capacity, first),
        [SM, VM, VM, VM],
        [VM] * 3,
        [vmem((slots, source_rows), BF16), vmem((2 * own_rows, slots), BF16), vmem((2 * moved, slots), BF16)],
        [],
        2 * column_tokens * column_tokens * 600,
        6 * slots * source_rows,
    )(me, spill_rows, ids_t, weight)

    def exchange(rows):
        shaped = rows.reshape(expert_count, -1, width)
        return lax.all_to_all(shaped, "expert", split_axis=0, concat_axis=0, tiled=True).reshape(-1, width)

    outbound = call(
        build_kernel,
        [VM] * (2 + peers),
        HB,
        hbm((cut, width), BF16),
        [vmem((cut, width), BF16), DMA((PIECES,))],
        2 * cut * source_rows * width,
        2 * (cut + source_rows) * width,
    )(pick[:cut], own, *arrived)
    inbound = exchange(outbound)
    size = rest // expert_count
    chips = expert_count // C
    blocks = call(
        functools.partial(build_blocks_kernel, C * size),
        [VM] * (2 + peers),
        [HB] * chips,
        [hbm((C * size, width), BF16)] * chips,
        [vmem((rest, width), BF16), DMA((chips,))],
        2 * rest * source_rows * width,
        2 * (rest + source_rows) * width,
    )(pick[cut:], own, *arrived)

    def far(k):
        z, y = k // (Y * C), k // C % Y
        return -(min(z, Z - z) + min(y, Y - y))

    landed = {0: in_hbm(blocks[0])}
    for j in sorted(range(1, chips), key=lambda j: far(j * C)):
        pairs = [(i, partner(i, j * C, 1)) for i in range(expert_count)]
        landed[j] = in_hbm(lax.ppermute(blocks[j], "expert", pairs))
    landed = [landed[j] for j in range(chips)]
    other = call(
        functools.partial(regroup_kernel, size),
        [HB] * chips,
        HB,
        hbm((chips * size, width), BF16),
        [vmem((chips * size, width), BF16), DMA((chips,)), DMA((1,))],
        1000 * rest * width,
        2 * rest * width,
    )(*landed)
    swapped = lax.ppermute(other, "expert", [(i, partner(i, 1, 1)) for i in range(expert_count)])
    arrivals = [*landed, in_hbm(swapped)]

    tiles, downs = ff // GATE_COLS, width // DOWN_COLS

    def experts(inputs, blocks, count, out_shape):
        return call(
            functools.partial(ffn_kernel, blocks, len(inputs)),
            [SM] + [HB] * (len(inputs) + 3),
            HB,
            hbm(out_shape, BF16),
            [
                vmem((count, width), BF16),
                vmem((tiles, width, 2 * GATE_COLS), BF16),
                vmem((downs, ff, DOWN_COLS), BF16),
                vmem((count, 2 * GATE_COLS), F32),
                vmem((count, ff), BF16),
                vmem((count, width), BF16),
                DMA((max(blocks, PIECES),)),
                DMA((PIECES, 2)),
                DMA((tiles, 2)),
                DMA((downs,)),
                DMA((max(blocks, downs),)),
            ],
            6 * count * width * ff,
            4 * count * width + 6 * width * ff,
            FFN_GRANT,
        )(me, *inputs, w_gate[0], w_up[0], w_down[0])

    outcome = experts([inbound], 1, cut, (cut, width))
    back0 = exchange(outcome)
    back1 = exchange(experts(arrivals, expert_count, rest, (expert_count, size, width)))

    part_own, part_arr = call(
        combine_first_kernel,
        [VM, VM, HB],
        [HB] * 2,
        [hbm((own_rows, width), F32), hbm((moved, width), F32)],
        [
            vmem((cut, width), BF16),
            vmem((own_rows, width), F32),
            vmem((moved, width), F32),
            DMA((PIECES,)),
            DMA((2 * PIECES,)),
        ],
        4 * source_rows * cut * width,
        2 * cut * width + 4 * source_rows * width,
    )(own_w[:, :cut], arr_w[:, :cut], in_hbm(back0))
    back1 = in_hbm(back1)
    arrived_parts = call(
        functools.partial(combine_arrived_kernel, room),
        [VM, HB, HB],
        [HB] * peers,
        [hbm((room, width), BF16)] * peers,
        [
            vmem((rest, width), BF16),
            vmem((moved, width), F32),
            vmem((moved, width), BF16),
            DMA((PIECES,)),
            DMA((PIECES,)),
            DMA((PIECES * peers,)),
        ],
        4 * moved * rest * width,
        2 * rest * width + 6 * moved * width,
    )(arr_w[:, cut:], back1, in_hbm(part_arr))
    returned = shift(arrived_parts, -1)
    own_part = call(
        combine_own_kernel,
        [VM, HB, HB],
        VM,
        vmem((own_rows, width), F32),
        [vmem((rest, width), BF16), vmem((own_rows, width), F32), DMA((PIECES,)), DMA((PIECES,))],
        4 * own_rows * rest * width,
        2 * rest * width + 8 * own_rows * width,
    )(own_w[:, cut:], back1, in_hbm(part_own))
    mixed = call(
        finish_kernel,
        [VM] * (2 + peers),
        HB,
        hbm((own_rows, width), BF16),
        [vmem((own_rows, width), BF16), DMA((PIECES,))],
        2 * moved * own_rows * width,
        8 * own_rows * width,
    )(give, own_part, *returned)
    return mixed[None]


def solution(mesh):
    in_specs = (
        P("expert", "dp", None),
        P("expert", None, None),
        P("expert", None, None),
        P("expert", None, None),
        P("expert", None, None),
        P("expert", None, None),
        P(),
        P("expert", None),
    )
    out_specs = P("expert", "dp", None)

    return jax.shard_map(local, mesh=mesh, in_specs=in_specs, out_specs=out_specs, check_vma=False)
```

```python
import functools
import jax
import jax.numpy as jnp
from jax import lax
from jax.experimental import pallas as pl
from jax.experimental.pallas import tpu as pltpu
from jax.sharding import PartitionSpec as P

F32 = jnp.float32
BF16 = jnp.bfloat16
I32 = jnp.int32


def onehot(mask):
    return jnp.where(mask, 1.0, 0.0).astype(BF16)


def strict_upper(n):
    return onehot(lax.broadcasted_iota(I32, (n, n), 0) < lax.broadcasted_iota(I32, (n, n), 1))


def dot(a, b):
    return jnp.dot(a, b, preferred_element_type=F32)


def dot_nt(a, b):
    return lax.dot_general(a, b, (((1,), (1,)), ((), ())), preferred_element_type=F32)


def dot_tn(a, b):
    return lax.dot_general(a, b, (((0,), (0,)), ((), ())), preferred_element_type=F32)


def send(buf_ref, out_ref, sems, j):
    return pltpu.make_async_copy(buf_ref, out_ref, sems.at[j])


def parts(width, count):
    step = width // count
    return [pl.ds(j * step, step) for j in range(count)]


PIECES = 4


def spill_kernel(dp_count, room, me_ref, spill_ref, tok_ref, pick_ref, own_ref, *refs):
    out_refs, (spill_buf, buf, spill_sem, in_sems, out_sems) = refs[: dp_count - 1], refs[dp_count - 1 :]
    own_rows, width = tok_ref.shape
    slots = pick_ref.shape[0]
    load = pltpu.make_async_copy(spill_ref, spill_buf, spill_sem)
    load.start()
    cols = parts(width, PIECES)
    loads = [send(tok_ref.at[:, c], own_ref.at[:, c], in_sems, j) for j, c in enumerate(cols)]
    for copy in loads:
        copy.start()
    load.wait()
    me = me_ref[0]
    senders = spill_buf[pl.ds(me, 1), :]
    peers = lax.broadcasted_iota(I32, (8, own_rows), 0)
    same = onehot(senders == peers)
    before = dot(same, strict_upper(own_rows))
    order = jnp.sum(before * same.astype(F32), axis=0, keepdims=True).astype(I32)
    ahead = jnp.where(senders < me, senders - me + dp_count, senders - me)
    target = jnp.where(ahead == 0, slots, (ahead - 1) * room + order)
    rows = lax.broadcasted_iota(I32, (slots, own_rows), 0)
    pick = onehot(rows == target)
    pick_ref[...] = pick
    stores = []
    for j, c in enumerate(cols):
        loads[j].wait()
        buf[:, c] = dot(pick, own_ref[:, c]).astype(BF16)
        for k, out_ref in enumerate(out_refs):
            store = send(buf.at[pl.ds(k * room, room), c], out_ref.at[:, c], out_sems, j * len(out_refs) + k)
            store.start()
            stores.append(store)
    for store in stores:
        store.wait()


Z, Y, C = 4, 4, 2


def partner(me, k, sign):
    z = (me // (Y * C) + sign * (k // (Y * C))) % Z
    y = (me // C % Y + sign * (k // C % Y)) % Y
    c = (me % C + k % C) % C
    return (z * Y + y) * C + c


def slot_of(index, experts_all, capacity, first):
    cut = experts_all * first
    in_first = index < cut
    expert = jnp.where(in_first, index // first, (index - cut) // (capacity - first))
    rank = jnp.where(in_first, index % first, first + (index - cut) % (capacity - first))
    return expert, rank + 1


def route_kernel(
    dp_count, room, experts_all, capacity, first, me_ref, spill_ref, ids_ref, weight_ref,
    pick_ref, own_w_ref, arr_w_ref
):
    me = me_ref[0]
    own_rows = spill_ref.shape[1]
    top_count, column_tokens = ids_ref.shape
    source_rows = own_rows + (dp_count - 1) * room
    slots = experts_all * capacity

    by_home = onehot(spill_ref[...] == me)
    order = dot(by_home, strict_upper(own_rows)).astype(I32)
    homes = lax.broadcasted_iota(I32, (dp_count, own_rows), 0)
    place = lax.broadcasted_iota(I32, (dp_count, own_rows), 1)
    back = jnp.where(homes > me, me - homes + dp_count, me - homes)
    row = jnp.where(back == 0, place, own_rows + (back - 1) * room + order)
    row = jnp.where(spill_ref[...] == me, row, source_rows)
    row = jnp.concatenate([row[h : h + 1] for h in range(dp_count)], axis=1)
    to_row = onehot(lax.broadcasted_iota(I32, (source_rows, column_tokens), 0) == row)

    experts = lax.broadcasted_iota(I32, (experts_all, column_tokens), 0)
    scale = jnp.zeros((experts_all, column_tokens), F32)
    chosen = jnp.zeros((experts_all, column_tokens), F32)
    mine = row < source_rows
    for k in range(top_count):
        hit = (ids_ref[k : k + 1, :] == experts) & mine
        scale = jnp.where(hit, weight_ref[k : k + 1, :], scale)
        chosen = jnp.where(hit, 1.0, chosen)
    rank = dot(chosen.astype(BF16), strict_upper(column_tokens))
    keep = (chosen > 0.0) & (rank < capacity)
    code = jnp.where(keep, rank + 1.0, 0.0).astype(BF16)
    scale = jnp.where(keep, scale, 0.0)
    high = scale.astype(BF16)
    low = (scale - high.astype(F32)).astype(BF16)

    slot_expert, _ = slot_of(lax.broadcasted_iota(I32, (slots, experts_all), 0), experts_all, capacity, first)
    slot_row = lax.broadcasted_iota(I32, (slots, experts_all), 0)
    slot_expert = jnp.where(slot_row < experts_all * first, slot_expert, partner(me_ref[1], slot_expert, 1))
    spread = onehot(slot_expert == lax.broadcasted_iota(I32, (slots, experts_all), 1))
    code_rows = dot_nt(code, to_row).astype(BF16)
    _, rank_col = slot_of(lax.broadcasted_iota(I32, (slots, source_rows), 0), experts_all, capacity, first)
    pick_ref[...] = onehot(dot(spread, code_rows).astype(I32) == rank_col)

    slot_expert, _ = slot_of(lax.broadcasted_iota(I32, (experts_all, slots), 1), experts_all, capacity, first)
    spread_t = onehot(slot_expert == lax.broadcasted_iota(I32, (experts_all, slots), 0))
    _, rank_row = slot_of(lax.broadcasted_iota(I32, (source_rows, slots), 1), experts_all, capacity, first)
    code_t = dot_nt(to_row, code).astype(BF16)
    filled = dot(code_t, spread_t).astype(I32) == rank_row
    high_t = dot(dot_nt(to_row, high).astype(BF16), spread_t)
    low_t = dot(dot_nt(to_row, low).astype(BF16), spread_t)
    high_w = jnp.where(filled, high_t, 0.0).astype(BF16)
    low_w = jnp.where(filled, low_t, 0.0).astype(BF16)
    own_w_ref[:own_rows] = high_w[:own_rows]
    own_w_ref[own_rows:] = low_w[:own_rows]
    arr_w_ref[: source_rows - own_rows] = high_w[own_rows:]
    arr_w_ref[source_rows - own_rows :] = low_w[own_rows:]


def build_kernel(pick_ref, *refs):
    *src_refs, out_ref, buf, sems = refs
    copies = []
    for j, c in enumerate(parts(out_ref.shape[1], PIECES)):
        rows = jnp.concatenate([ref[:, c] for ref in src_refs], axis=0)
        buf[:, c] = dot(pick_ref[...], rows).astype(BF16)
        copies.append(send(buf.at[:, c], out_ref.at[:, c], sems, j))
        copies[-1].start()
    for copy in copies:
        copy.wait()


def build_blocks_kernel(size, pick_ref, *refs):
    count = pick_ref.shape[0] // size
    src_refs, out_refs, (buf, sems) = refs[: -count - 2], refs[-count - 2 : -2], refs[-2:]
    for c in parts(buf.shape[1], PIECES):
        rows = jnp.concatenate([ref[:, c] for ref in src_refs], axis=0)
        buf[:, c] = dot(pick_ref[...], rows).astype(BF16)
    copies = [send(buf.at[pl.ds(k * size, size)], out_ref, sems, k) for k, out_ref in enumerate(out_refs)]
    for copy in copies:
        copy.start()
    for copy in copies:
        copy.wait()


def regroup_kernel(size, *refs):
    *in_refs, out_ref, buf, in_sems, out_sem = refs
    loads = [send(ref.at[pl.ds(size, size)], buf.at[pl.ds(j * size, size)], in_sems, j) for j, ref in enumerate(in_refs)]
    for load in loads:
        load.start()
    for load in loads:
        load.wait()
    store = send(buf, out_ref, out_sem, 0)
    store.start()
    store.wait()


GATE_COLS = 128
DOWN_COLS = 1024


def ffn_kernel(blocks, inputs, me_ref, *refs):
    x_in, (gate_in, up_in, down_in, out_ref, x, both, down, acc, hidden, buf) = refs[:inputs], refs[inputs : inputs + 10]
    x_sem, top_sem, both_sem, down_sem, out_sem = refs[inputs + 10 :]
    depth = x.shape[1] // PIECES
    tiles, downs = both.shape[0], down.shape[0]
    size = x.shape[0] // blocks

    def lanes(n, step):
        return pl.ds(pl.multiple_of(n * step, step), step)

    def fetch(n):
        cols = lanes(n, GATE_COLS)
        return (
            pltpu.make_async_copy(gate_in.at[:, cols], both.at[n, :, pl.ds(0, GATE_COLS)], both_sem.at[n, 0]),
            pltpu.make_async_copy(up_in.at[:, cols], both.at[n, :, pl.ds(GATE_COLS, GATE_COLS)], both_sem.at[n, 1]),
        )

    def fetch_down(n):
        return pltpu.make_async_copy(down_in.at[:, lanes(n, DOWN_COLS)], down.at[n], down_sem.at[n])

    def store(n):
        cols = lanes(n, DOWN_COLS)
        return pltpu.make_async_copy(buf.at[:, cols], out_ref.at[:, cols], out_sem.at[n])

    def activate(n):
        gate_part, up_part = acc[:, :GATE_COLS], acc[:, GATE_COLS:]
        hidden[:, lanes(n, GATE_COLS)] = (jax.nn.silu(gate_part) * up_part).astype(BF16)

    def top(k):
        d = lanes(k, depth)
        rows = [] if blocks > 1 else [pltpu.make_async_copy(x_in[0].at[:, d], x.at[:, d], x_sem.at[k])]
        return rows + [
            pltpu.make_async_copy(gate_in.at[d, pl.ds(0, GATE_COLS)], both.at[0, d, pl.ds(0, GATE_COLS)], top_sem.at[k, 0]),
            pltpu.make_async_copy(up_in.at[d, pl.ds(0, GATE_COLS)], both.at[0, d, pl.ds(GATE_COLS, GATE_COLS)], top_sem.at[k, 1]),
        ]

    whole = []
    if blocks > 1:
        for k in range(blocks):
            chip, core = k // C, k % C
            ref, row = (x_in[-1], chip * size) if core else (x_in[chip], 0)
            whole.append(send(ref.at[pl.ds(row, size)], x.at[pl.ds(k * size, size)], x_sem, k))
    for copy in whole:
        copy.start()
    for k in range(PIECES):
        for copy in top(k):
            copy.start()
    for copy in whole:
        copy.wait()
    acc[...] = jnp.zeros_like(acc)

    @pl.loop(0, PIECES)
    def _(k):
        for copy in top(k):
            copy.wait()
        for ahead in (1, 2):

            @pl.when(k == 2 * ahead - 1)
            def _():
                for copy in fetch(ahead):
                    copy.start()

        d = lanes(k, depth)
        acc[...] += dot(x[:, d], both[0, d, :])

    activate(0)

    @pl.loop(1, tiles)
    def _(n):
        for copy in fetch(n):
            copy.wait()

        @pl.when(n + 2 < tiles)
        def _():
            for copy in fetch(n + 2):
                copy.start()

        @pl.when(n + 2 >= tiles)
        def _():
            half = (n + 2 - tiles) * (downs // 2)
            for j in range(downs // 2):
                fetch_down(half + j).start()

        acc[...] = dot(x[...], both[n])
        activate(n)

    @pl.loop(0, downs)
    def _(n):
        fetch_down(n).wait()
        buf[:, lanes(n, DOWN_COLS)] = dot(hidden[...], down[n]).astype(BF16)
        if blocks == 1:
            store(n).start()

    if blocks == 1:

        @pl.loop(0, downs)
        def _(n):
            store(n).wait()

    else:
        stores = []
        for k in range(blocks):
            home = partner(me_ref[1], k, -1)
            stores.append(send(buf.at[pl.ds(k * size, size)], out_ref.at[home], out_sem, k))
            stores[-1].start()
        for copy in stores:
            copy.wait()


def weighted(w_ref, res):
    both = dot(w_ref[...], res)
    half = both.shape[0] // 2
    return both[:half] + both[half:]


def each_piece(res_ref, res, sems):
    cols = parts(res.shape[1], PIECES)
    loads = [send(res_ref.at[:, c], res.at[:, c], sems, j) for j, c in enumerate(cols)]
    for load in loads:
        load.start()
    for j, c in enumerate(cols):
        loads[j].wait()
        yield j, c


def combine_first_kernel(own_w_ref, arr_w_ref, res_ref, own_ref, arr_ref, res, own_buf, arr_buf, in_sems, sems):
    copies = []
    for j, c in each_piece(res_ref, res, in_sems):
        own_buf[:, c] = weighted(own_w_ref, res[:, c])
        arr_buf[:, c] = weighted(arr_w_ref, res[:, c])
        copies.append(send(own_buf.at[:, c], own_ref.at[:, c], sems, 2 * j))
        copies.append(send(arr_buf.at[:, c], arr_ref.at[:, c], sems, 2 * j + 1))
        copies[-2].start()
        copies[-1].start()
    for copy in copies:
        copy.wait()


def with_part(part_ref, part, part_sems):
    return each_piece(part_ref, part, part_sems)


def combine_own_kernel(w_ref, res_ref, part_ref, out_ref, part, part_sems):
    for _, c in with_part(part_ref, part, part_sems):
        out_ref[:, c] = part[:, c] + weighted(w_ref, res_ref[:, c])


def combine_arrived_kernel(room, w_ref, res_ref, part_ref, *refs):
    *out_refs, part, buf, part_sems, sems = refs
    copies = []
    for j, c in with_part(part_ref, part, part_sems):
        buf[:, c] = (part[:, c] + weighted(w_ref, res_ref[:, c])).astype(BF16)
        for k, out_ref in enumerate(out_refs):
            copies.append(send(buf.at[pl.ds(k * room, room), c], out_ref.at[:, c], sems, j * len(out_refs) + k))
            copies[-1].start()
    for copy in copies:
        copy.wait()


def finish_kernel(pick_ref, own_ref, *refs):
    *back_refs, out_ref, buf, sems = refs
    copies = []
    for j, c in enumerate(parts(out_ref.shape[1], PIECES)):
        back = jnp.concatenate([ref[:, c] for ref in back_refs], axis=0)
        buf[:, c] = (own_ref[:, c] + dot_tn(pick_ref[...], back)).astype(BF16)
        copies.append(send(buf.at[:, c], out_ref.at[:, c], sems, j))
        copies[-1].start()
    for copy in copies:
        copy.wait()


GRANT = 24 * 1024 * 1024
FFN_GRANT = 56 * 1024 * 1024


def in_hbm(x):
    return pltpu.with_memory_space_constraint(x, pltpu.HBM)


VM = pl.BlockSpec(memory_space=pltpu.VMEM)
SM = pl.BlockSpec(memory_space=pltpu.SMEM)
HB = pl.BlockSpec(memory_space=pltpu.HBM)
DMA = pltpu.SemaphoreType.DMA


def call(kernel, in_specs, out_specs, out_shape, scratch, flops, size, grant=GRANT):
    return pl.pallas_call(
        kernel,
        in_specs=in_specs,
        out_specs=out_specs,
        out_shape=out_shape,
        scratch_shapes=scratch,
        compiler_params=pltpu.CompilerParams(vmem_limit_bytes=grant),
        cost_estimate=pl.CostEstimate(flops=flops, bytes_accessed=size, transcendentals=0),
    )


def local(tokens, w_gate, w_up, w_down, expert_ids, gate_index, gate_table, spill):
    dp_count = lax.axis_size("dp")
    expert_count = lax.axis_size("expert")
    own_rows, width = tokens.shape[1:]
    column_tokens = spill.shape[1]
    top_count = expert_ids.shape[2]
    experts_all = w_gate.shape[0] * expert_count
    capacity = 3 * own_rows * top_count // (2 * experts_all)
    room = own_rows // 4
    moved = (dp_count - 1) * room
    source_rows = own_rows + moved
    slots = experts_all * capacity
    ff = w_gate.shape[2]
    first = capacity - 8
    cut = experts_all * first
    rest = slots - cut
    me = jnp.stack([lax.axis_index("dp"), lax.axis_index("expert")]).astype(I32)
    own_in = in_hbm(tokens[0])
    spill_rows = spill.reshape(dp_count, own_rows)
    hbm, vmem = pltpu.HBM, pltpu.VMEM
    steps = range(1, dp_count)
    peers = len(steps)

    def shift(blocks, sign):
        sent = {}
        for k in sorted(steps, key=lambda k: abs(dp_count - 2 * k)):
            pairs = [(i, (i + sign * k) % dp_count) for i in range(dp_count)]
            sent[k] = lax.ppermute(blocks[k - 1], "dp", pairs)
        return [sent[k] for k in steps]

    give, own, *outgoing = call(
        functools.partial(spill_kernel, dp_count, room),
        [SM, HB, HB],
        [VM, VM] + [HB] * peers,
        [vmem((moved, own_rows), BF16), vmem((own_rows, width), BF16)] + [hbm((room, width), BF16)] * peers,
        [vmem((dp_count, own_rows), I32), vmem((moved, width), BF16), DMA(()), DMA((PIECES,)), DMA((PIECES * peers,))],
        2 * moved * own_rows * width,
        4 * own_rows * width,
    )(me, in_hbm(spill_rows), own_in)
    arrived = shift(outgoing, 1)

    level_count = gate_table.shape[0]
    index_t = gate_index[0].T
    ids_t = expert_ids[0].T
    matches = index_t[:, None, :] == jnp.arange(level_count, dtype=I32)[None, :, None]
    picked = jnp.sum(jnp.where(matches, gate_table[None, :, None], 0.0), axis=1)
    weight = picked / jnp.sum(picked, axis=0, keepdims=True)
    pick, own_w, arr_w = call(
        functools.partial(route_kernel, dp_count, room, experts_all, capacity, first),
        [SM, VM, VM, VM],
        [VM] * 3,
        [vmem((slots, source_rows), BF16), vmem((2 * own_rows, slots), BF16), vmem((2 * moved, slots), BF16)],
        [],
        2 * column_tokens * column_tokens * 600,
        6 * slots * source_rows,
    )(me, spill_rows, ids_t, weight)

    def exchange(rows):
        shaped = rows.reshape(expert_count, -1, width)
        return lax.all_to_all(shaped, "expert", split_axis=0, concat_axis=0, tiled=True).reshape(-1, width)

    outbound = call(
        build_kernel,
        [VM] * (2 + peers),
        HB,
        hbm((cut, width), BF16),
        [vmem((cut, width), BF16), DMA((PIECES,))],
        2 * cut * source_rows * width,
        2 * (cut + source_rows) * width,
    )(pick[:cut], own, *arrived)
    inbound = exchange(outbound)
    size = rest // expert_count
    chips = expert_count // C
    blocks = call(
        functools.partial(build_blocks_kernel, C * size),
        [VM] * (2 + peers),
        [HB] * chips,
        [hbm((C * size, width), BF16)] * chips,
        [vmem((rest, width), BF16), DMA((chips,))],
        2 * rest * source_rows * width,
        2 * (rest + source_rows) * width,
    )(pick[cut:], own, *arrived)

    def far(k):
        z, y = k // (Y * C), k // C % Y
        return -(min(z, Z - z) + min(y, Y - y))

    landed = {0: in_hbm(blocks[0])}
    for j in sorted(range(1, chips), key=lambda j: far(j * C)):
        pairs = [(i, partner(i, j * C, 1)) for i in range(expert_count)]
        landed[j] = in_hbm(lax.ppermute(blocks[j], "expert", pairs))
    landed = [landed[j] for j in range(chips)]
    other = call(
        functools.partial(regroup_kernel, size),
        [HB] * chips,
        HB,
        hbm((chips * size, width), BF16),
        [vmem((chips * size, width), BF16), DMA((chips,)), DMA((1,))],
        1000 * rest * width,
        2 * rest * width,
    )(*landed)
    swapped = lax.ppermute(other, "expert", [(i, partner(i, 1, 1)) for i in range(expert_count)])
    arrivals = [*landed, in_hbm(swapped)]

    tiles, downs = ff // GATE_COLS, width // DOWN_COLS

    def experts(inputs, blocks, count, out_shape):
        return call(
            functools.partial(ffn_kernel, blocks, len(inputs)),
            [SM] + [HB] * (len(inputs) + 3),
            HB,
            hbm(out_shape, BF16),
            [
                vmem((count, width), BF16),
                vmem((tiles, width, 2 * GATE_COLS), BF16),
                vmem((downs, ff, DOWN_COLS), BF16),
                vmem((count, 2 * GATE_COLS), F32),
                vmem((count, ff), BF16),
                vmem((count, width), BF16),
                DMA((max(blocks, PIECES),)),
                DMA((PIECES, 2)),
                DMA((tiles, 2)),
                DMA((downs,)),
                DMA((max(blocks, downs),)),
            ],
            6 * count * width * ff,
            4 * count * width + 6 * width * ff,
            FFN_GRANT,
        )(me, *inputs, w_gate[0], w_up[0], w_down[0])

    outcome = experts([inbound], 1, cut, (cut, width))
    back0 = exchange(outcome)
    back1 = exchange(experts(arrivals, expert_count, rest, (expert_count, size, width)))

    part_own, part_arr = call(
        combine_first_kernel,
        [VM, VM, HB],
        [HB] * 2,
        [hbm((own_rows, width), F32), hbm((moved, width), F32)],
        [
            vmem((cut, width), BF16),
            vmem((own_rows, width), F32),
            vmem((moved, width), F32),
            DMA((PIECES,)),
            DMA((2 * PIECES,)),
        ],
        4 * source_rows * cut * width,
        2 * cut * width + 4 * source_rows * width,
    )(own_w[:, :cut], arr_w[:, :cut], in_hbm(back0))
    arrived_parts = call(
        functools.partial(combine_arrived_kernel, room),
        [VM, VM, HB],
        [HB] * peers,
        [hbm((room, width), BF16)] * peers,
        [
            vmem((moved, width), F32),
            vmem((moved, width), BF16),
            DMA((PIECES,)),
            DMA((PIECES * peers,)),
        ],
        4 * moved * rest * width,
        2 * rest * width + 6 * moved * width,
    )(arr_w[:, cut:], back1, in_hbm(part_arr))
    returned = shift(arrived_parts, -1)
    own_part = call(
        combine_own_kernel,
        [VM, VM, HB],
        VM,
        vmem((own_rows, width), F32),
        [vmem((own_rows, width), F32), DMA((PIECES,))],
        4 * own_rows * rest * width,
        2 * rest * width + 8 * own_rows * width,
    )(own_w[:, cut:], back1, in_hbm(part_own))
    mixed = call(
        finish_kernel,
        [VM] * (2 + peers),
        HB,
        hbm((own_rows, width), BF16),
        [vmem((own_rows, width), BF16), DMA((PIECES,))],
        2 * moved * own_rows * width,
        8 * own_rows * width,
    )(give, own_part, *returned)
    return mixed[None]


def solution(mesh):
    in_specs = (
        P("expert", "dp", None),
        P("expert", None, None),
        P("expert", None, None),
        P("expert", None, None),
        P("expert", None, None),
        P("expert", None, None),
        P(),
        P("expert", None),
    )
    out_specs = P("expert", "dp", None)

    return jax.shard_map(local, mesh=mesh, in_specs=in_specs, out_specs=out_specs, check_vma=False)
```
